256 devices in a mesh: streams: 16 (over z_lo, x), tm: 16 (over z_hi, y, core).
Axes of the slice: x: 4, y: 4, z: 8 (z_hi: 2, z_lo: 4; z = z_hi * 4 + z_lo), core: 2. Of those that a mesh axis runs over, the one named last changes fastest.
Arguments:
- signal: float32 [2, 16777216], P(None, ('streams', 'tm')), parts along dimension 1, may hold values from -6 to 6
- coarse_taps: float32 [16, 64], replicated, may hold values from -1.5 to 1.5
- fine_taps: float32 [12, 512], replicated, may hold values from -1.8 to 1.8
Outputs:
- channelized: float32 [2, 64, 512, 512], P(None, 'tm', 'streams'), parts along dimension 2
The draws below stay inside these ranges and needn't reach their ends.
There are 16 independent parts, one for each index of `streams`. The reference program is written for one: setup_inputs(seed, part) draws one part's arguments, and reference() takes and returns one part's arrays. A program takes and returns all parts, laid end to end along the dimension named above; an argument that names none is the same for every part. Nothing has to cross between parts.
All inputs are finite; a program needn't handle non-finite values.
Results may differ from the reference program's by a relative error of at most 0.00007.
Values sent between devices are 32-bit elements; how exact they have to be, the bound alone decides.
A program may use at most 320 MiB of HBM per device.

```python
import math
import jax
import jax.numpy as jnp
from jax import lax

CHANNELS = 64
FINE = 512
TAPS = 16
FINE_TAPS = 12
SAMPLES = 1048576
FRAMES = 16384
FINE_FRAMES = 32


def steps_of(rng, dims, cuts, low, largest):
    def one(dim, blocks):
        steps = jax.random.uniform(jax.random.fold_in(jax.random.fold_in(rng, 6), dim), (blocks,), jnp.float32, low / len(cuts), largest / len(cuts))
        return jnp.repeat(jnp.exp(steps), dims[dim] // blocks).reshape((-1,) + (1,) * (len(dims) - dim - 1))

    factor_of = one(*cuts[0])
    for cut in cuts[1:]:
        factor_of = factor_of * one(*cut)
    return factor_of


def noise(own_key, dims, deviation, most, cuts=(), kind=jnp.bfloat16):
    loudness = steps_of(own_key, dims, cuts, -0.22, 0.18) if cuts else 1.0
    result = jax.random.normal(own_key, dims, jnp.float32) * deviation * loudness
    return jnp.minimum(jnp.maximum(result, -most), most).astype(kind)


def setup_inputs(seed: int = 0, part: int = 0) -> dict:
    keys = jax.random.split(jax.random.key(seed), 4)
    own_keys = jax.random.split(jax.random.fold_in(keys[3], part), 4)
    signal = noise(own_keys[0], (2, SAMPLES), 1.0, 6.0, ((1, 16),), jnp.float32)
    coarse_taps = noise(keys[1], (TAPS, CHANNELS), 0.25, 1.5, (), jnp.float32)
    fine_taps = noise(keys[2], (FINE_TAPS, FINE), 0.3, 1.8, (), jnp.float32)
    return dict(signal=signal, coarse_taps=coarse_taps, fine_taps=fine_taps)


def tables(points):
    counter = jnp.arange(points, dtype=jnp.int32)
    product = counter[:, None] * counter[None, :] % points
    angle = product.astype(jnp.float32) * (2.0 * math.pi / points)
    return (jnp.cos(angle), jnp.sin(angle))

def spectrum_last(real_part, imag_part, points):
    cosine_table, sine_table = tables(points)
    factor = 1.0 / math.sqrt(points)
    highest = lax.Precision.HIGHEST
    out_real = (jnp.matmul(real_part, cosine_table, precision=highest) + jnp.matmul(imag_part, sine_table, precision=highest)) * factor
    out_imag = (jnp.matmul(imag_part, cosine_table, precision=highest) - jnp.matmul(real_part, sine_table, precision=highest)) * factor
    return jnp.stack([out_real, out_imag])

def reference(signal, coarse_taps, fine_taps):
    framed = signal.reshape(2, FRAMES, CHANNELS)
    padded = jnp.pad(framed, ((0, 0), (TAPS - 1, 0), (0, 0)))
    branches = jnp.zeros((2, FRAMES, CHANNELS), jnp.float32)
    for tap_index in range(TAPS):
        offset = TAPS - 1 - tap_index
        branches = branches + coarse_taps[tap_index] * padded[:, offset:offset + FRAMES, :]
    coarse = spectrum_last(branches[0], branches[1], CHANNELS)
    coarse = jnp.transpose(coarse, (0, 2, 1)).reshape(2, CHANNELS, FINE_FRAMES, FINE)
    padded_fine = jnp.pad(coarse, ((0, 0), (0, 0), (FINE_TAPS - 1, 0), (0, 0)))
    fine_branches = jnp.zeros((2, CHANNELS, FINE_FRAMES, FINE), jnp.float32)
    for tap_index in range(FINE_TAPS):
        offset = FINE_TAPS - 1 - tap_index
        fine_branches = fine_branches + fine_taps[tap_index] * padded_fine[:, :, offset:offset + FINE_FRAMES, :]
    return spectrum_last(fine_branches[0], fine_branches[1], FINE)
```

```python
import functools
import math

import jax
import jax.numpy as jnp
import numpy as np
from jax import lax
from jax.experimental import pallas as pl
from jax.experimental.pallas import tpu as pltpu
from jax.sharding import Mesh
from jax.sharding import PartitionSpec as P

CHANNELS = 64
FINE = 512
TAPS = 16
FINE_TAPS = 12
TM = ("zh", "y", "c")
GROUP = (2, 4, 2)
PEERS = 16
LANES = 128
HALO = 16
ROWS = 1024
HALF = 512
MESH = pl.DeviceIdType.MESH
OTHERS = [
    (dz, dy, dc)
    for dz in (1, 0)
    for dy in (2, 1, 3, 0)
    for dc in (1, 0)
    if (dz, dy, dc) != (0, 0, 0)
]


def split(value):
    high = value.astype(jnp.bfloat16)
    low = (value - high.astype(jnp.float32)).astype(jnp.bfloat16)
    return high, low


def np_split(value):
    value = value.astype(np.float32)
    high = value.astype(jnp.bfloat16)
    low = (value - high.astype(np.float32)).astype(jnp.bfloat16)
    return high, low


def coarse_matrix():
    owner, part, own, parity = np.meshgrid(
        np.arange(16), np.arange(2), np.arange(4), np.arange(2), indexing="ij"
    )
    channel = (4 * owner + own).reshape(-1, 1)
    part, parity = part.reshape(-1, 1), parity.reshape(-1, 1)
    part_in, parity_in, branch = np.meshgrid(
        np.arange(2), np.arange(2), np.arange(CHANNELS), indexing="ij"
    )
    part_in, parity_in, branch = (v.reshape(1, -1) for v in (part_in, parity_in, branch))
    angle = 2.0 * np.pi * (channel * branch % CHANNELS) / CHANNELS
    value = np.where(part == part_in, np.cos(angle), np.sin(angle) * (part_in - part))
    value = np.where(parity == parity_in, value, 0.0) / math.sqrt(CHANNELS)
    high, low = np_split(value)
    return np.concatenate([high, low, high], axis=1)


def fine_matrix():
    part_in, b = np.meshgrid(np.arange(2), np.arange(LANES), indexing="ij")
    part_in, b = part_in.reshape(-1, 1), b.reshape(-1, 1)
    part, c = part_in.reshape(1, -1), b.reshape(1, -1)
    angle = 2.0 * np.pi * (b * c % LANES) / LANES
    value = np.where(part == part_in, np.cos(angle), np.sin(angle) * (part_in - part))
    high, low = np_split(value / math.sqrt(FINE))
    return np.concatenate([high, low, high], axis=0)


def twiddles():
    a, c = np.meshgrid(np.arange(4), np.arange(LANES), indexing="ij")
    angle = 2.0 * np.pi * a * c / FINE
    return np.concatenate([np.cos(angle), np.sin(angle)]).astype(np.float32)


def place():
    return tuple(lax.axis_index(a) for a in TM)


def shifted(me, by):
    return tuple(lax.rem(m + d, n) for m, d, n in zip(me, by, GROUP, strict=True))


def flat(at):
    return (at[0] * 4 + at[1]) * 2 + at[2]


def named(at):
    return dict(zip(TM, at, strict=True))


def gather_kernel(
    x_hbm, m_hbm, ct_hbm, ft_hbm, got, taps_out,
    xs, ys, ms, ct, ft, ftt, sent, load_sem, halo_sem, send_sem, recv_sem,
):
    me = place()
    mine = flat(me)
    barrier = pltpu.get_barrier_semaphore()
    for by in OTHERS:
        pl.semaphore_signal(barrier, inc=1, device_id=named(shifted(me, by)), device_id_type=MESH)
    loads = [
        pltpu.make_async_copy(x_hbm, xs.at[pl.ds(HALO, ROWS)], load_sem.at[0]),
        pltpu.make_async_copy(m_hbm, ms, load_sem.at[1]),
        pltpu.make_async_copy(ct_hbm, ct, load_sem.at[2]),
        pltpu.make_async_copy(ft_hbm, ft, load_sem.at[3]),
    ]
    for load in loads:
        load.start()
    loads[2].wait()
    taps = ct[...]
    taps = jnp.concatenate([taps, taps], axis=1)
    loads[0].wait()
    loads[1].wait()

    def delay(start, size):
        first = lax.broadcasted_iota(jnp.int32, (size, LANES), 1) < CHANNELS
        here = xs[pl.ds(start, size), :]
        before = xs[pl.ds(start - 2, size), :]
        ys[pl.ds(start, size), :] = pltpu.roll(jnp.where(first, here, before), CHANNELS, 1)

    def filtered(m):
        pieces = []
        for a1 in range(2):
            for c in range(2):
                acc = None
                for i in range(TAPS // 2):
                    at = HALO + HALF * m + 2 * a1 + c - 2 * i
                    rows = pl.ds(at, LANES, stride=4)
                    term = taps[2 * i : 2 * i + 1] * xs[rows, :]
                    acc = term if acc is None else acc + term
                    acc = acc + taps[2 * i + 1 : 2 * i + 2] * ys[rows, :]
                pieces.append(acc)
        full = jnp.concatenate(
            [
                jnp.concatenate(pieces[0:2], axis=1),
                jnp.concatenate(pieces[2:4], axis=1),
            ],
            axis=0,
        )
        high, low = split(full)
        right = jnp.concatenate([high, high, low], axis=1)
        result = lax.dot_general(
            ms[...], right, (((1,), (1,)), ((), ())), preferred_element_type=jnp.float32
        )
        sent[m] = result.reshape(PEERS, 16, 256)
        got[m, mine] = sent[m, mine]

    def send(m):
        copies = []
        for k, by in enumerate(OTHERS):
            to = shifted(me, by)
            copy = pltpu.make_async_remote_copy(
                src_ref=sent.at[m, flat(to)],
                dst_ref=got.at[m, mine],
                send_sem=send_sem.at[m, k],
                recv_sem=recv_sem.at[m, k],
                device_id=named(to),
                device_id_type=MESH,
            )
            copy.start()
            copies.append(copy)
        return copies

    delay(HALO + HALF - 16, HALF + 16)
    filtered(1)
    pl.semaphore_wait(barrier, len(OTHERS))
    last = mine == PEERS - 1
    after = lax.rem(mine + 1, PEERS)
    halo = pltpu.make_async_remote_copy(
        src_ref=xs.at[pl.ds(ROWS, HALO)],
        dst_ref=xs.at[pl.ds(0, HALO)],
        send_sem=halo_sem.at[0],
        recv_sem=halo_sem.at[1],
        device_id=named((after // 8, lax.rem(after // 2, 4), lax.rem(after, 2))),
        device_id_type=MESH,
    )

    @pl.when(jnp.logical_not(last))
    def _():
        halo.start()

    copies = send(1)

    @pl.when(mine == 0)
    def _():
        xs[pl.ds(0, HALO), :] = jnp.zeros((HALO, LANES), jnp.float32)

    @pl.when(mine > 0)
    def _():
        halo.wait_recv()

    delay(2, HALF + HALO - 16 - 2)
    filtered(0)
    copies += send(0)

    loads[3].wait()
    square = jnp.concatenate([ft[...], jnp.zeros((LANES - FINE_TAPS, FINE), jnp.float32)], axis=0)
    for k in range(4):
        ftt[pl.ds(LANES * k, LANES), :] = square[:, LANES * k : LANES * (k + 1)].T
    by_branch = [ftt[pl.ds(a, LANES, stride=4), :].T for a in range(4)]
    odd = lax.rem(lax.broadcasted_iota(jnp.int32, (8, LANES), 0), 2) == 1
    for a1 in range(2):
        for j in range(FINE_TAPS):
            even_row = jnp.broadcast_to(by_branch[2 * a1][j : j + 1], (8, LANES))
            odd_row = jnp.broadcast_to(by_branch[2 * a1 + 1][j : j + 1], (8, LANES))
            taps_out[a1, j] = jnp.where(odd, odd_row, even_row)

    for copy in copies:
        copy.wait()

    @pl.when(jnp.logical_not(last))
    def _():
        halo.wait_send()


def fine_kernel(got, taps, cm, tw, out, fir, stage, out_sem):
    for a1 in range(2):
        for c in range(2):
            for frame in range(32):
                acc = None
                for j in range(min(FINE_TAPS, frame + 1)):
                    at = frame - j
                    block = got[at % 2, at // 2, pl.ds(8 * c, 8), pl.ds(LANES * a1, LANES)]
                    term = taps[a1, j] * block
                    acc = term if acc is None else acc + term
                fir[a1, c, pl.ds(8 * frame, 8), :] = acc
    cosine = tw[pl.ds(0, 4), :]
    sine = tw[pl.ds(4, 4), :]
    writes = []
    for k in range(4):
        rows = []
        for a in range(4):
            parts = [fir[a // 2, c, pl.ds(2 * k + a % 2, 32, stride=8), :] for c in range(2)]
            rows.append(jnp.concatenate(parts, axis=1))
        left = jnp.concatenate(rows, axis=0)
        high, low = split(left)
        left = jnp.concatenate([high, high, low], axis=1)
        spectrum = jnp.dot(left, cm[...], preferred_element_type=jnp.float32)
        real, imag = [], []
        for a in range(4):
            re = spectrum[32 * a : 32 * a + 32, :LANES]
            im = spectrum[32 * a : 32 * a + 32, LANES:]
            if a:
                cos, sin = cosine[a : a + 1], sine[a : a + 1]
                re, im = re * cos + im * sin, im * cos - re * sin
            real.append(re)
            imag.append(im)
        sum_re, sum_im = real[0] + real[2], imag[0] + imag[2]
        dif_re, dif_im = real[0] - real[2], imag[0] - imag[2]
        odd_re, odd_im = real[1] + real[3], imag[1] + imag[3]
        off_re, off_im = real[1] - real[3], imag[1] - imag[3]
        stage[k, 0, :, 0:128] = sum_re + odd_re
        stage[k, 1, :, 0:128] = sum_im + odd_im
        stage[k, 0, :, 128:256] = dif_re + off_im
        stage[k, 1, :, 128:256] = dif_im - off_re
        stage[k, 0, :, 256:384] = sum_re - odd_re
        stage[k, 1, :, 256:384] = sum_im - odd_im
        stage[k, 0, :, 384:512] = dif_re - off_im
        stage[k, 1, :, 384:512] = dif_im + off_re
        for c in range(2):
            write = pltpu.make_async_copy(stage.at[k, c], out.at[c, k], out_sem.at[k, c])
            write.start()
            writes.append(write)
    for write in writes:
        write.wait()


def on_device(signal, coarse_taps, fine_taps):
    rows = signal.reshape(2, HALF, LANES).transpose(1, 0, 2).reshape(ROWS, LANES)
    anywhere = pl.BlockSpec(memory_space=pl.ANY)
    vmem = pl.BlockSpec(memory_space=pltpu.VMEM)
    got, taps = pl.pallas_call(
        gather_kernel,
        out_shape=[
            jax.ShapeDtypeStruct((2, PEERS, 16, 256), jnp.float32),
            jax.ShapeDtypeStruct((2, FINE_TAPS, 8, LANES), jnp.float32),
        ],
        in_specs=[anywhere] * 4,
        out_specs=[vmem, vmem],
        scratch_shapes=[
            pltpu.VMEM((HALO + ROWS, LANES), jnp.float32),
            pltpu.VMEM((HALO + ROWS, LANES), jnp.float32),
            pltpu.VMEM((256, 768), jnp.bfloat16),
            pltpu.VMEM((TAPS, CHANNELS), jnp.float32),
            pltpu.VMEM((FINE_TAPS, FINE), jnp.float32),
            pltpu.VMEM((FINE, LANES), jnp.float32),
            pltpu.VMEM((2, PEERS, 16, 256), jnp.float32),
            pltpu.SemaphoreType.DMA((4,)),
            pltpu.SemaphoreType.DMA((2,)),
            pltpu.SemaphoreType.DMA((2, len(OTHERS))),
            pltpu.SemaphoreType.DMA((2, len(OTHERS))),
        ],
        compiler_params=pltpu.CompilerParams(collective_id=0, has_side_effects=True),
        name="gather",
    )(rows, jnp.asarray(coarse_matrix()), coarse_taps, fine_taps)
    return pl.pallas_call(
        fine_kernel,
        out_shape=jax.ShapeDtypeStruct((2, 4, 32, FINE), jnp.float32),
        in_specs=[vmem] * 4,
        out_specs=anywhere,
        scratch_shapes=[
            pltpu.VMEM((2, 2, 256, LANES), jnp.float32),
            pltpu.VMEM((4, 2, 32, FINE), jnp.float32),
            pltpu.SemaphoreType.DMA((4, 2)),
        ],
        name="fine",
    )(got, taps, jnp.asarray(fine_matrix()), jnp.asarray(twiddles()))


def solution(mesh):
    finer = Mesh(mesh.devices.reshape(mesh.shape["streams"], *GROUP), ("streams", *TM))
    return jax.shard_map(
        on_device,
        mesh=finer,
        in_specs=(P(None, ("streams", *TM)), P(), P()),
        out_specs=P(None, TM, "streams", None),
        check_vma=False,
    )
```

```python
import functools
import math

import jax
import jax.numpy as jnp
import numpy as np
from jax import lax
from jax.experimental import pallas as pl
from jax.experimental.pallas import tpu as pltpu
from jax.sharding import Mesh
from jax.sharding import PartitionSpec as P

CHANNELS = 64
FINE = 512
TAPS = 16
FINE_TAPS = 12
TM = ("zh", "y", "c")
GROUP = (2, 4, 2)
PEERS = 16
LANES = 128
HEAD = 16
TAIL = 32
ROWS = 1024
HALF = 512
MESH = pl.DeviceIdType.MESH
OTHERS = [
    (dz, dy, dc)
    for dz in (1, 0)
    for dy in (2, 1, 3, 0)
    for dc in (1, 0)
    if (dz, dy, dc) != (0, 0, 0)
]


def split(value):
    high = value.astype(jnp.bfloat16)
    low = (value - high.astype(jnp.float32)).astype(jnp.bfloat16)
    return high, low


def np_split(value):
    value = value.astype(np.float32)
    high = value.astype(jnp.bfloat16)
    low = (value - high.astype(np.float32)).astype(jnp.bfloat16)
    return high, low


def coarse_matrix():
    owner, part, own, parity = np.meshgrid(
        np.arange(16), np.arange(2), np.arange(4), np.arange(2), indexing="ij"
    )
    channel = (4 * owner + own).reshape(-1, 1)
    part, parity = part.reshape(-1, 1), parity.reshape(-1, 1)
    part_in, parity_in, branch = np.meshgrid(
        np.arange(2), np.arange(2), np.arange(CHANNELS), indexing="ij"
    )
    part_in, parity_in, branch = (v.reshape(1, -1) for v in (part_in, parity_in, branch))
    angle = 2.0 * np.pi * (channel * branch % CHANNELS) / CHANNELS
    value = np.where(part == part_in, np.cos(angle), np.sin(angle) * (part_in - part))
    value = np.where(parity == parity_in, value, 0.0) / math.sqrt(CHANNELS)
    high, low = np_split(value)
    return np.concatenate([high, low, high], axis=1)


def fine_matrix():
    part_in, b = np.meshgrid(np.arange(2), np.arange(LANES), indexing="ij")
    part_in, b = part_in.reshape(-1, 1), b.reshape(-1, 1)
    part, c = part_in.reshape(1, -1), b.reshape(1, -1)
    angle = 2.0 * np.pi * (b * c % LANES) / LANES
    value = np.where(part == part_in, np.cos(angle), np.sin(angle) * (part_in - part))
    high, low = np_split(value / math.sqrt(FINE))
    return np.concatenate([high, low, high], axis=0)


def twiddles():
    a, c = np.meshgrid(np.arange(4), np.arange(LANES), indexing="ij")
    angle = 2.0 * np.pi * a * c / FINE
    return np.concatenate([np.cos(angle), np.sin(angle)]).astype(np.float32)


def place():
    return tuple(lax.axis_index(a) for a in TM)


def shifted(me, by):
    return tuple(lax.rem(m + d, n) for m, d, n in zip(me, by, GROUP, strict=True))


def flat(at):
    return (at[0] * 4 + at[1]) * 2 + at[2]


def named(at):
    return dict(zip(TM, at, strict=True))


def coarse_frames(xs, ys, taps, start, size):
    parts = []
    for c in range(2):
        acc = None
        for i in range(TAPS // 2):
            rows = pl.ds(HEAD + start + c - 2 * i, size, stride=4)
            term = taps[2 * i : 2 * i + 1] * xs[rows, :]
            acc = term if acc is None else acc + term
            acc = acc + taps[2 * i + 1 : 2 * i + 2] * ys[rows, :]
        parts.append(acc)
    return jnp.concatenate(parts, axis=1)


def spectra(ms, frames):
    high, low = split(frames)
    right = jnp.concatenate([high, high, low], axis=1)
    return lax.dot_general(
        ms[...], right, (((1,), (1,)), ((), ())), preferred_element_type=jnp.float32
    )


def fine_filter(a1, block, taps, fir):
    for c in range(2):
        for frame in range(32):
            acc = None
            for j in range(min(FINE_TAPS, frame + 1)):
                term = taps(j) * block(c, frame - j)
                acc = term if acc is None else acc + term
            fir[c, pl.ds(8 * frame, 8), :] = acc


def fine_spectra(a1, k, fir, cm, tw):
    rows = []
    for h in range(2):
        parts = [fir[c, pl.ds(2 * k + h, 32, stride=8), :] for c in range(2)]
        rows.append(jnp.concatenate(parts, axis=1))
    high, low = split(jnp.concatenate(rows, axis=0))
    left = jnp.concatenate([high, high, low], axis=1)
    spectrum = jnp.dot(left, cm[...], preferred_element_type=jnp.float32)
    result = []
    for h in range(2):
        a = 2 * a1 + h
        re = spectrum[32 * h : 32 * h + 32, :LANES]
        im = spectrum[32 * h : 32 * h + 32, LANES:]
        if a:
            cos, sin = tw[a : a + 1, :], tw[4 + a : 5 + a, :]
            re, im = re * cos + im * sin, im * cos - re * sin
        result.append((re, im))
    return result


def gather_kernel(
    x_hbm, m_hbm, ct_hbm, ft_hbm, c_hbm, t_hbm, got, extra, taps_out, first, cm, tw,
    xs, ys, ms, ct, ft, ftt, early, tails, heads, sent, fir,
    load_sem, send_sem, recv_sem,
):
    me = place()
    mine = flat(me)
    barrier = pltpu.get_barrier_semaphore()
    for by in OTHERS:
        pl.semaphore_signal(barrier, inc=1, device_id=named(shifted(me, by)), device_id_type=MESH)
    loads = [
        pltpu.make_async_copy(x_hbm, xs.at[pl.ds(HEAD, ROWS)], load_sem.at[0]),
        pltpu.make_async_copy(ct_hbm, ct, load_sem.at[1]),
        pltpu.make_async_copy(m_hbm, ms, load_sem.at[2]),
        pltpu.make_async_copy(ft_hbm, ft, load_sem.at[3]),
        pltpu.make_async_copy(c_hbm, cm, load_sem.at[4]),
        pltpu.make_async_copy(t_hbm, tw, load_sem.at[5]),
    ]
    for load in loads:
        load.start()
    xs[pl.ds(0, HEAD), :] = jnp.zeros((HEAD, LANES), jnp.float32)
    xs[pl.ds(HEAD + ROWS, TAIL), :] = jnp.zeros((TAIL, LANES), jnp.float32)
    ys[pl.ds(0, HEAD), :] = jnp.zeros((HEAD, LANES), jnp.float32)
    loads[1].wait()
    taps = ct[...]
    taps = jnp.concatenate([taps, taps], axis=1)
    loads[0].wait()
    loads[2].wait()

    size = ROWS + TAIL
    left = lax.broadcasted_iota(jnp.int32, (size, LANES), 1) < CHANNELS
    here = xs[pl.ds(HEAD, size), :]
    before = xs[pl.ds(HEAD - 2, size), :]
    ys[pl.ds(HEAD, size), :] = pltpu.roll(jnp.where(left, here, before), CHANNELS, 1)

    def compute(a1):
        frames = [coarse_frames(xs, ys, taps, HALF * m + 2 * a1, LANES) for m in range(2)]
        result = spectra(ms, jnp.concatenate(frames, axis=0))
        sent[a1] = result.reshape(PEERS, 16, 256)

    def send(piece, source, target):
        copies = []
        for k, by in enumerate(OTHERS):
            to = shifted(me, by)
            copy = pltpu.make_async_remote_copy(
                src_ref=source.at[flat(to)],
                dst_ref=target.at[mine],
                send_sem=send_sem.at[piece, k],
                recv_sem=recv_sem.at[piece, k],
                device_id=named(to),
                device_id_type=MESH,
            )
            copy.start()
            copies.append(copy)
        return copies

    compute(0)
    early[mine] = sent[0, mine]
    pl.semaphore_wait(barrier, len(OTHERS))
    copies = [send(0, sent.at[0], early)]
    compute(1)
    got[mine] = sent[1, mine]
    copies.append(send(1, sent.at[1], got))

    ends = [coarse_frames(xs, ys, taps, ROWS + 2 * a1, 8) for a1 in range(2)]
    lower = lax.broadcasted_iota(jnp.int32, (8, 256), 0) < 4
    ends = jnp.where(lower, ends[0], pltpu.roll(ends[1], 4, 0))
    result = spectra(ms, jnp.concatenate([ends] * 16, axis=0))
    chosen = (
        lax.broadcasted_iota(jnp.int32, (16, LANES), 1) // 8
        == lax.broadcasted_iota(jnp.int32, (16, LANES), 0)
    )
    for d in range(PEERS):
        picked = jnp.where(chosen, result[16 * d : 16 * d + 16], 0.0)
        tails[d] = jnp.sum(picked, axis=0, keepdims=True)
    heads[mine] = tails[mine]
    copies.append(send(2, tails, heads))

    loads[3].wait()
    square = jnp.concatenate([ft[...], jnp.zeros((LANES - FINE_TAPS, FINE), jnp.float32)], axis=0)
    for k in range(4):
        ftt[pl.ds(LANES * k, LANES), :] = square[:, LANES * k : LANES * (k + 1)].T
    by_branch = [ftt[pl.ds(a, LANES, stride=4), :].T for a in range(4)]
    odd = lax.rem(lax.broadcasted_iota(jnp.int32, (8, LANES), 0), 2) == 1
    for a1 in range(2):
        for j in range(FINE_TAPS):
            even_row = jnp.broadcast_to(by_branch[2 * a1][j : j + 1], (8, LANES))
            odd_row = jnp.broadcast_to(by_branch[2 * a1 + 1][j : j + 1], (8, LANES))
            taps_out[a1, j] = jnp.where(odd, odd_row, even_row)
    loads[4].wait()
    loads[5].wait()

    for copy in copies[2]:
        copy.wait_recv()
    spread = jnp.concatenate(
        [jnp.where(chosen, jnp.broadcast_to(heads[s], (16, LANES)), 0.0) for s in range(PEERS)],
        axis=0,
    )
    row = lax.rem(lax.broadcasted_iota(jnp.int32, (256, 256), 0), 8)
    column = lax.broadcasted_iota(jnp.int32, (256, 256), 1)
    lane = lax.rem(column, LANES)
    select = jnp.logical_and(lane < 4, row == column // LANES * 4 + lane)
    added = jnp.dot(
        jnp.concatenate(split(spread), axis=1),
        jnp.where(select, 1.0, 0.0).astype(jnp.bfloat16),
        preferred_element_type=jnp.float32,
    )
    extra[...] = added[:, LANES:].reshape(PEERS, 16, LANES)

    for copy in copies[0]:
        copy.wait_recv()
    for s in range(1, PEERS):
        early[s, :, 0:LANES] += added[16 * s - 16 : 16 * s, :LANES]
    fine_filter(
        0,
        lambda c, f: early[f // 2, pl.ds(8 * c, 8), pl.ds(LANES * (f % 2), LANES)],
        lambda j: taps_out[0, j],
        fir,
    )
    for k in range(4):
        for h, parts in enumerate(fine_spectra(0, k, fir, cm, tw)):
            for c in range(2):
                first[k, h, c] = parts[c]

    for copy in copies[1]:
        copy.wait_recv()
    for piece in copies:
        for copy in piece:
            copy.wait_send()


def fine_kernel(got, extra, taps, first, cm, tw, out, fir, stage, out_sem):
    blocks = {}

    def block(c, frame):
        if (c, frame) not in blocks:
            value = got[frame // 2, pl.ds(8 * c, 8), pl.ds(LANES * (frame % 2), LANES)]
            if frame % 2 == 0 and frame > 0:
                value = value + extra[frame // 2 - 1, pl.ds(8 * c, 8), :]
            blocks[c, frame] = value
        return blocks[c, frame]

    fine_filter(1, block, lambda j: taps[1, j], fir)
    writes = []
    for k in range(4):
        (re1, im1), (re3, im3) = fine_spectra(1, k, fir, cm, tw)
        re0, im0, re2, im2 = first[k, 0, 0], first[k, 0, 1], re1, im1
        re1, im1 = first[k, 1, 0], first[k, 1, 1]
        sum_re, sum_im = re0 + re2, im0 + im2
        dif_re, dif_im = re0 - re2, im0 - im2
        odd_re, odd_im = re1 + re3, im1 + im3
        off_re, off_im = re1 - re3, im1 - im3
        stage[k, 0, :, 0:128] = sum_re + odd_re
        stage[k, 1, :, 0:128] = sum_im + odd_im
        stage[k, 0, :, 128:256] = dif_re + off_im
        stage[k, 1, :, 128:256] = dif_im - off_re
        stage[k, 0, :, 256:384] = sum_re - odd_re
        stage[k, 1, :, 256:384] = sum_im - odd_im
        stage[k, 0, :, 384:512] = dif_re - off_im
        stage[k, 1, :, 384:512] = dif_im + off_re
        for c in range(2):
            write = pltpu.make_async_copy(stage.at[k, c], out.at[c, k], out_sem.at[k, c])
            write.start()
            writes.append(write)
    for write in writes:
        write.wait()


def on_device(signal, coarse_taps, fine_taps):
    rows = signal.reshape(2, HALF, LANES).transpose(1, 0, 2).reshape(ROWS, LANES)
    hbm = pl.BlockSpec(memory_space=pltpu.HBM)
    vmem = pl.BlockSpec(memory_space=pltpu.VMEM)
    tables = [jnp.asarray(v) for v in (coarse_matrix(), fine_matrix(), twiddles())]
    operands = (rows, tables[0], coarse_taps, fine_taps, *tables[1:])
    f32 = jnp.float32
    handed = pl.pallas_call(
        gather_kernel,
        out_shape=[
            jax.ShapeDtypeStruct((PEERS, 16, 256), f32),
            jax.ShapeDtypeStruct((PEERS, 16, LANES), f32),
            jax.ShapeDtypeStruct((2, FINE_TAPS, 8, LANES), f32),
            jax.ShapeDtypeStruct((4, 2, 2, 32, LANES), f32),
            jax.ShapeDtypeStruct((768, 256), jnp.bfloat16),
            jax.ShapeDtypeStruct((8, LANES), f32),
        ],
        in_specs=[hbm] * 6,
        out_specs=[vmem] * 6,
        scratch_shapes=[
            pltpu.VMEM((HEAD + ROWS + TAIL, LANES), f32),
            pltpu.VMEM((HEAD + ROWS + TAIL, LANES), f32),
            pltpu.VMEM((256, 768), jnp.bfloat16),
            pltpu.VMEM((TAPS, CHANNELS), f32),
            pltpu.VMEM((FINE_TAPS, FINE), f32),
            pltpu.VMEM((FINE, LANES), f32),
            pltpu.VMEM((PEERS, 16, 256), f32),
            pltpu.VMEM((PEERS, 1, LANES), f32),
            pltpu.VMEM((PEERS, 1, LANES), f32),
            pltpu.VMEM((2, PEERS, 16, 256), f32),
            pltpu.VMEM((2, 256, LANES), f32),
            pltpu.SemaphoreType.DMA((6,)),
            pltpu.SemaphoreType.DMA((3, len(OTHERS))),
            pltpu.SemaphoreType.DMA((3, len(OTHERS))),
        ],
        compiler_params=pltpu.CompilerParams(
            collective_id=0, has_side_effects=True, vmem_limit_bytes=16 << 20
        ),
        name="gather",
    )(*(pltpu.with_memory_space_constraint(v, pltpu.HBM) for v in operands))
    return pl.pallas_call(
        fine_kernel,
        out_shape=jax.ShapeDtypeStruct((2, 4, 32, FINE), f32),
        in_specs=[vmem] * 6,
        out_specs=hbm,
        scratch_shapes=[
            pltpu.VMEM((2, 256, LANES), f32),
            pltpu.VMEM((4, 2, 32, FINE), f32),
            pltpu.SemaphoreType.DMA((4, 2)),
        ],
        compiler_params=pltpu.CompilerParams(vmem_limit_bytes=16 << 20),
        name="fine",
    )(*handed)


def solution(mesh):
    finer = Mesh(mesh.devices.reshape(mesh.shape["streams"], *GROUP), ("streams", *TM))
    return jax.shard_map(
        on_device,
        mesh=finer,
        in_specs=(P(None, ("streams", *TM)), P(), P()),
        out_specs=P(None, TM, "streams", None),
        check_vma=False,
    )
```

```python
import functools
import math

import jax
import jax.numpy as jnp
import numpy as np
from jax import lax
from jax.experimental import pallas as pl
from jax.experimental.pallas import tpu as pltpu
from jax.sharding import Mesh
from jax.sharding import PartitionSpec as P

CHANNELS = 64
FINE = 512
TAPS = 16
FINE_TAPS = 12
TM = ("zh", "y", "c")
GROUP = (2, 4, 2)
PEERS = 16
LANES = 128
HEAD = 16
TAIL = 32
ROWS = 1024
HALF = 512
MESH = pl.DeviceIdType.MESH
ACROSS = [(y, c) for y in (0, 1, 3, 2) for c in (1, 0)]
BESIDE = [(dy, dc) for dy in (2, 1, 3, 0) for dc in (1, 0) if (dy, dc) != (0, 0)]


def split(value):
    high = value.astype(jnp.bfloat16)
    low = (value - high.astype(jnp.float32)).astype(jnp.bfloat16)
    return high, low


def np_split(value):
    value = value.astype(np.float32)
    high = value.astype(jnp.bfloat16)
    low = (value - high.astype(np.float32)).astype(jnp.bfloat16)
    return high, low


def coarse_matrix():
    owner, part, own, parity = np.meshgrid(
        np.arange(16), np.arange(2), np.arange(4), np.arange(2), indexing="ij"
    )
    channel = (4 * owner + own).reshape(-1, 1)
    part, parity = part.reshape(-1, 1), parity.reshape(-1, 1)
    part_in, parity_in, branch = np.meshgrid(
        np.arange(2), np.arange(2), np.arange(CHANNELS), indexing="ij"
    )
    part_in, parity_in, branch = (v.reshape(1, -1) for v in (part_in, parity_in, branch))
    angle = 2.0 * np.pi * (channel * branch % CHANNELS) / CHANNELS
    value = np.where(part == part_in, np.cos(angle), np.sin(angle) * (part_in - part))
    value = np.where(parity == parity_in, value, 0.0) / math.sqrt(CHANNELS)
    high, low = np_split(value)
    return np.concatenate([high, low, high], axis=1)


def fine_matrix():
    part_in, b = np.meshgrid(np.arange(2), np.arange(LANES), indexing="ij")
    part_in, b = part_in.reshape(-1, 1), b.reshape(-1, 1)
    part, c = part_in.reshape(1, -1), b.reshape(1, -1)
    angle = 2.0 * np.pi * (b * c % LANES) / LANES
    value = np.where(part == part_in, np.cos(angle), np.sin(angle) * (part_in - part))
    high, low = np_split(value / math.sqrt(FINE))
    return np.concatenate([high, low, high], axis=0)


def twiddles():
    a, c = np.meshgrid(np.arange(4), np.arange(LANES), indexing="ij")
    angle = 2.0 * np.pi * a * c / FINE
    return np.concatenate([np.cos(angle), np.sin(angle)]).astype(np.float32)


def flat(zh, y, c):
    return (zh * 4 + y) * 2 + c


def named(zh, y, c):
    return {"zh": zh, "y": y, "c": c}


def coarse_frames(xs, ys, taps, start, size):
    parts = []
    for c in range(2):
        acc = None
        for i in range(TAPS // 2):
            rows = pl.ds(HEAD + start + c - 2 * i, size, stride=4)
            term = taps[2 * i : 2 * i + 1] * xs[rows, :]
            acc = term if acc is None else acc + term
            acc = acc + taps[2 * i + 1 : 2 * i + 2] * ys[rows, :]
        parts.append(acc)
    return jnp.concatenate(parts, axis=1)


def spectra(ms, frames):
    high, low = split(frames)
    right = jnp.concatenate([high, high, low], axis=1)
    return lax.dot_general(
        ms[...], right, (((1,), (1,)), ((), ())), preferred_element_type=jnp.float32
    )


def fine_filter(a1, block, taps, fir):
    for c in range(2):
        for frame in range(32):
            acc = None
            for j in range(min(FINE_TAPS, frame + 1)):
                term = taps(j) * block(c, frame - j)
                acc = term if acc is None else acc + term
            fir[c, pl.ds(8 * frame, 8), :] = acc


def fine_spectra(a1, k, fir, cm, tw):
    rows = []
    for h in range(2):
        parts = [fir[c, pl.ds(2 * k + h, 32, stride=8), :] for c in range(2)]
        rows.append(jnp.concatenate(parts, axis=1))
    high, low = split(jnp.concatenate(rows, axis=0))
    left = jnp.concatenate([high, high, low], axis=1)
    spectrum = jnp.dot(left, cm[...], preferred_element_type=jnp.float32)
    result = []
    for h in range(2):
        a = 2 * a1 + h
        re = spectrum[32 * h : 32 * h + 32, :LANES]
        im = spectrum[32 * h : 32 * h + 32, LANES:]
        if a:
            cos, sin = tw[a : a + 1, :], tw[4 + a : 5 + a, :]
            re, im = re * cos + im * sin, im * cos - re * sin
        result.append((re, im))
    return result


def gather_kernel(
    x_hbm, m_hbm, ct_hbm, ft_hbm, c_hbm, t_hbm, got, extra, taps_out, first, cm, tw,
    xs, ys, ms, ct, ft, ftt, early, tails, heads, sent, fir,
    load_sem, send_sem, recv_sem, ready, again,
):
    zh, y, c = (lax.axis_index(axis) for axis in TM)
    mine = flat(zh, y, c)
    own = 2 * y + c
    other = 1 - zh
    late = zh == 1
    held = jnp.logical_and(late, lax.axis_index("streams") // 4 == 3)
    barrier = pltpu.get_barrier_semaphore()
    for at in ACROSS:
        pl.semaphore_signal(barrier, inc=1, device_id=named(other, *at), device_id_type=MESH)
    loads = [
        pltpu.make_async_copy(x_hbm, xs.at[pl.ds(HEAD, ROWS)], load_sem.at[0]),
        pltpu.make_async_copy(ct_hbm, ct, load_sem.at[1]),
        pltpu.make_async_copy(m_hbm, ms, load_sem.at[2]),
        pltpu.make_async_copy(ft_hbm, ft, load_sem.at[3]),
        pltpu.make_async_copy(c_hbm, cm, load_sem.at[4]),
        pltpu.make_async_copy(t_hbm, tw, load_sem.at[5]),
    ]
    for load in loads:
        load.start()

    @pl.when(late)
    def _():
        pl.semaphore_wait(barrier, len(ACROSS))
        for at in ACROSS:
            pl.semaphore_signal(
                ready.at[own], inc=1, device_id=named(other, *at), device_id_type=MESH
            )

    xs[pl.ds(0, HEAD), :] = jnp.zeros((HEAD, LANES), jnp.float32)
    xs[pl.ds(HEAD + ROWS, TAIL), :] = jnp.zeros((TAIL, LANES), jnp.float32)
    ys[pl.ds(0, HEAD), :] = jnp.zeros((HEAD, LANES), jnp.float32)
    loads[1].wait()
    taps = ct[...]
    taps = jnp.concatenate([taps, taps], axis=1)
    loads[0].wait()
    loads[2].wait()

    size = ROWS + TAIL
    left = lax.broadcasted_iota(jnp.int32, (size, LANES), 1) < CHANNELS
    here = xs[pl.ds(HEAD, size), :]
    before = xs[pl.ds(HEAD - 2, size), :]
    ys[pl.ds(HEAD, size), :] = pltpu.roll(jnp.where(left, here, before), CHANNELS, 1)

    def compute(a1):
        frames = [coarse_frames(xs, ys, taps, HALF * m + 2 * a1, LANES) for m in range(2)]
        result = spectra(ms, jnp.concatenate(frames, axis=0))
        sent[a1] = result.reshape(PEERS, 16, 256)

    def crossing(piece, source, target):
        return [
            pltpu.make_async_remote_copy(
                src_ref=source.at[flat(other, *at)],
                dst_ref=target.at[mine],
                send_sem=send_sem.at[piece, flat(0, *at)],
                recv_sem=recv_sem.at[piece, own],
                device_id=named(other, *at),
                device_id_type=MESH,
            )
            for at in ACROSS
        ]

    def staying(piece, source, target):
        copies = []
        for k, (dy, dc) in enumerate(BESIDE):
            to = (zh, lax.rem(y + dy, 4), lax.rem(c + dc, 2))
            copy = pltpu.make_async_remote_copy(
                src_ref=source.at[flat(*to)],
                dst_ref=target.at[mine],
                send_sem=send_sem.at[piece, 8 + k],
                recv_sem=recv_sem.at[piece, 8 + k],
                device_id=named(*to),
                device_id_type=MESH,
            )
            copies.append(copy)
        return copies

    def arrived(piece, target, first, count):
        for k in range(first, first + count):
            pltpu.make_async_remote_copy(
                src_ref=target.at[0],
                dst_ref=target.at[0],
                send_sem=send_sem.at[piece, k],
                recv_sem=recv_sem.at[piece, k],
                device_id=named(other, y, c),
                device_id_type=MESH,
            ).wait_recv()

    compute(0)
    zero = crossing(0, sent.at[0], early)
    for at, copy in zip(ACROSS, zero, strict=True):

        @pl.when(jnp.logical_not(late))
        def _():
            pl.semaphore_wait(ready.at[flat(0, *at)], 1)

        copy.start()

    @pl.when(jnp.logical_not(late))
    def _():
        pl.semaphore_wait(barrier, len(ACROSS))
        pl.semaphore_signal(again, inc=1, device_id=named(other, y, c), device_id_type=MESH)

    early[mine] = sent[0, mine]

    ends = [coarse_frames(xs, ys, taps, ROWS + 2 * a1, 8) for a1 in range(2)]
    lower = lax.broadcasted_iota(jnp.int32, (8, 256), 0) < 4
    ends = jnp.where(lower, ends[0], pltpu.roll(ends[1], 4, 0))
    result = spectra(ms, jnp.concatenate([ends] * 16, axis=0))
    chosen = (
        lax.broadcasted_iota(jnp.int32, (16, LANES), 1) // 8
        == lax.broadcasted_iota(jnp.int32, (16, LANES), 0)
    )
    for d in range(PEERS):
        picked = jnp.where(chosen, result[16 * d : 16 * d + 16], 0.0)
        tails[d] = jnp.sum(picked, axis=0, keepdims=True)
    heads[mine] = tails[mine]
    two = crossing(2, tails, heads)
    for copy in two:
        copy.start()

    compute(1)
    got[mine] = sent[1, mine]
    one = crossing(1, sent.at[1], got)

    @pl.when(jnp.logical_not(held))
    def _():
        for copy in one:
            copy.start()

    @pl.when(late)
    def _():
        pl.semaphore_wait(again, 1)

    near = [
        *staying(0, sent.at[0], early),
        *staying(2, tails, heads),
        *staying(1, sent.at[1], got),
    ]
    for copy in near:
        copy.start()

    loads[3].wait()
    square = jnp.concatenate([ft[...], jnp.zeros((LANES - FINE_TAPS, FINE), jnp.float32)], axis=0)
    for k in range(4):
        ftt[pl.ds(LANES * k, LANES), :] = square[:, LANES * k : LANES * (k + 1)].T
    by_branch = [ftt[pl.ds(a, LANES, stride=4), :].T for a in range(4)]
    odd = lax.rem(lax.broadcasted_iota(jnp.int32, (8, LANES), 0), 2) == 1
    for a1 in range(2):
        for j in range(FINE_TAPS):
            even_row = jnp.broadcast_to(by_branch[2 * a1][j : j + 1], (8, LANES))
            odd_row = jnp.broadcast_to(by_branch[2 * a1 + 1][j : j + 1], (8, LANES))
            taps_out[a1, j] = jnp.where(odd, odd_row, even_row)
    loads[4].wait()
    loads[5].wait()

    arrived(0, early, 0, 8)

    @pl.when(held)
    def _():
        for copy in one:
            copy.start()

    arrived(0, early, 8, 7)
    arrived(2, heads, 0, 15)
    spread = jnp.concatenate(
        [jnp.where(chosen, jnp.broadcast_to(heads[s], (16, LANES)), 0.0) for s in range(PEERS)],
        axis=0,
    )
    row = lax.rem(lax.broadcasted_iota(jnp.int32, (256, 256), 0), 8)
    column = lax.broadcasted_iota(jnp.int32, (256, 256), 1)
    lane = lax.rem(column, LANES)
    select = jnp.logical_and(lane < 4, row == column // LANES * 4 + lane)
    added = jnp.dot(
        jnp.concatenate(split(spread), axis=1),
        jnp.where(select, 1.0, 0.0).astype(jnp.bfloat16),
        preferred_element_type=jnp.float32,
    )
    extra[...] = added[:, LANES:].reshape(PEERS, 16, LANES)

    for s in range(1, PEERS):
        early[s, :, 0:LANES] += added[16 * s - 16 : 16 * s, :LANES]
    fine_filter(
        0,
        lambda c, f: early[f // 2, pl.ds(8 * c, 8), pl.ds(LANES * (f % 2), LANES)],
        lambda j: taps_out[0, j],
        fir,
    )
    for k in range(4):
        for h, parts in enumerate(fine_spectra(0, k, fir, cm, tw)):
            for c in range(2):
                first[k, h, c] = parts[c]

    arrived(1, got, 0, 15)
    for copy in (*zero, *two, *one, *near):
        copy.wait_send()


def fine_kernel(got, extra, taps, first, cm, tw, out, fir, stage, out_sem):
    blocks = {}

    def block(c, frame):
        if (c, frame) not in blocks:
            value = got[frame // 2, pl.ds(8 * c, 8), pl.ds(LANES * (frame % 2), LANES)]
            if frame % 2 == 0 and frame > 0:
                value = value + extra[frame // 2 - 1, pl.ds(8 * c, 8), :]
            blocks[c, frame] = value
        return blocks[c, frame]

    fine_filter(1, block, lambda j: taps[1, j], fir)
    writes = []
    for k in range(4):
        (re1, im1), (re3, im3) = fine_spectra(1, k, fir, cm, tw)
        re0, im0, re2, im2 = first[k, 0, 0], first[k, 0, 1], re1, im1
        re1, im1 = first[k, 1, 0], first[k, 1, 1]
        sum_re, sum_im = re0 + re2, im0 + im2
        dif_re, dif_im = re0 - re2, im0 - im2
        odd_re, odd_im = re1 + re3, im1 + im3
        off_re, off_im = re1 - re3, im1 - im3
        stage[k, 0, :, 0:128] = sum_re + odd_re
        stage[k, 1, :, 0:128] = sum_im + odd_im
        stage[k, 0, :, 128:256] = dif_re + off_im
        stage[k, 1, :, 128:256] = dif_im - off_re
        stage[k, 0, :, 256:384] = sum_re - odd_re
        stage[k, 1, :, 256:384] = sum_im - odd_im
        stage[k, 0, :, 384:512] = dif_re - off_im
        stage[k, 1, :, 384:512] = dif_im + off_re
        for c in range(2):
            write = pltpu.make_async_copy(stage.at[k, c], out.at[c, k], out_sem.at[k, c])
            write.start()
            writes.append(write)
    for write in writes:
        write.wait()


def on_device(signal, coarse_taps, fine_taps):
    rows = signal.reshape(2, HALF, LANES).transpose(1, 0, 2).reshape(ROWS, LANES)
    hbm = pl.BlockSpec(memory_space=pltpu.HBM)
    vmem = pl.BlockSpec(memory_space=pltpu.VMEM)
    tables = [jnp.asarray(v) for v in (coarse_matrix(), fine_matrix(), twiddles())]
    operands = (rows, tables[0], coarse_taps, fine_taps, *tables[1:])
    f32 = jnp.float32
    handed = pl.pallas_call(
        gather_kernel,
        out_shape=[
            jax.ShapeDtypeStruct((PEERS, 16, 256), f32),
            jax.ShapeDtypeStruct((PEERS, 16, LANES), f32),
            jax.ShapeDtypeStruct((2, FINE_TAPS, 8, LANES), f32),
            jax.ShapeDtypeStruct((4, 2, 2, 32, LANES), f32),
            jax.ShapeDtypeStruct((768, 256), jnp.bfloat16),
            jax.ShapeDtypeStruct((8, LANES), f32),
        ],
        in_specs=[hbm] * 6,
        out_specs=[vmem] * 6,
        scratch_shapes=[
            pltpu.VMEM((HEAD + ROWS + TAIL, LANES), f32),
            pltpu.VMEM((HEAD + ROWS + TAIL, LANES), f32),
            pltpu.VMEM((256, 768), jnp.bfloat16),
            pltpu.VMEM((TAPS, CHANNELS), f32),
            pltpu.VMEM((FINE_TAPS, FINE), f32),
            pltpu.VMEM((FINE, LANES), f32),
            pltpu.VMEM((PEERS, 16, 256), f32),
            pltpu.VMEM((PEERS, 1, LANES), f32),
            pltpu.VMEM((PEERS, 1, LANES), f32),
            pltpu.VMEM((2, PEERS, 16, 256), f32),
            pltpu.VMEM((2, 256, LANES), f32),
            pltpu.SemaphoreType.DMA((6,)),
            pltpu.SemaphoreType.DMA((3, 15)),
            pltpu.SemaphoreType.DMA((3, 15)),
            pltpu.SemaphoreType.REGULAR((8,)),
            pltpu.SemaphoreType.REGULAR,
        ],
        compiler_params=pltpu.CompilerParams(
            collective_id=0, has_side_effects=True, vmem_limit_bytes=16 << 20
        ),
        name="gather",
    )(*(pltpu.with_memory_space_constraint(v, pltpu.HBM) for v in operands))
    return pl.pallas_call(
        fine_kernel,
        out_shape=jax.ShapeDtypeStruct((2, 4, 32, FINE), f32),
        in_specs=[vmem] * 6,
        out_specs=hbm,
        scratch_shapes=[
            pltpu.VMEM((2, 256, LANES), f32),
            pltpu.VMEM((4, 2, 32, FINE), f32),
            pltpu.SemaphoreType.DMA((4, 2)),
        ],
        compiler_params=pltpu.CompilerParams(vmem_limit_bytes=16 << 20),
        name="fine",
    )(*handed)


def solution(mesh):
    finer = Mesh(mesh.devices.reshape(mesh.shape["streams"], *GROUP), ("streams", *TM))
    return jax.shard_map(
        on_device,
        mesh=finer,
        in_specs=(P(None, ("streams", *TM)), P(), P()),
        out_specs=P(None, TM, "streams", None),
        check_vma=False,
    )
```

```python
import functools
import math

import jax
import jax.numpy as jnp
import numpy as np
from jax import lax
from jax.experimental import pallas as pl
from jax.experimental.pallas import tpu as pltpu
from jax.sharding import Mesh
from jax.sharding import PartitionSpec as P

CHANNELS = 64
FINE = 512
TAPS = 16
FINE_TAPS = 12
TM = ("zh", "y", "c")
GROUP = (2, 4, 2)
PEERS = 16
LANES = 128
HEAD = 16
TAIL = 32
ROWS = 1024
HALF = 512
MESH = pl.DeviceIdType.MESH
BESIDE = [(dy, dc) for dy in (2, 1, 3, 0) for dc in (1, 0) if (dy, dc) != (0, 0)]


def split(value):
    high = value.astype(jnp.bfloat16)
    low = (value - high.astype(jnp.float32)).astype(jnp.bfloat16)
    return high, low


def np_split(value):
    value = value.astype(np.float32)
    high = value.astype(jnp.bfloat16)
    low = (value - high.astype(np.float32)).astype(jnp.bfloat16)
    return high, low


def coarse_matrix():
    owner, part, own, parity = np.meshgrid(
        np.arange(16), np.arange(2), np.arange(4), np.arange(2), indexing="ij"
    )
    channel = (4 * owner + own).reshape(-1, 1)
    part, parity = part.reshape(-1, 1), parity.reshape(-1, 1)
    part_in, parity_in, branch = np.meshgrid(
        np.arange(2), np.arange(2), np.arange(CHANNELS), indexing="ij"
    )
    part_in, parity_in, branch = (v.reshape(1, -1) for v in (part_in, parity_in, branch))
    angle = 2.0 * np.pi * (channel * branch % CHANNELS) / CHANNELS
    value = np.where(part == part_in, np.cos(angle), np.sin(angle) * (part_in - part))
    value = np.where(parity == parity_in, value, 0.0) / math.sqrt(CHANNELS)
    return np.concatenate(np_split(value), axis=1)


def fine_matrix():
    part_in, b = np.meshgrid(np.arange(2), np.arange(LANES), indexing="ij")
    part_in, b = part_in.reshape(-1, 1), b.reshape(-1, 1)
    part, c = part_in.reshape(1, -1), b.reshape(1, -1)
    angle = 2.0 * np.pi * (b * c % LANES) / LANES
    value = np.where(part == part_in, np.cos(angle), np.sin(angle) * (part_in - part))
    high, low = np_split(value / math.sqrt(FINE))
    return np.concatenate([high, low, high], axis=0)


def twiddles():
    a, c = np.meshgrid(np.arange(4), np.arange(LANES), indexing="ij")
    angle = 2.0 * np.pi * a * c / FINE
    return np.concatenate([np.cos(angle), np.sin(angle)]).astype(np.float32)


def flat(zh, y, c):
    return (zh * 4 + y) * 2 + c


def named(zh, y, c):
    return {"zh": zh, "y": y, "c": c}


def coarse_frames(xs, ys, taps, start, size):
    parts = []
    for c in range(2):
        acc = None
        for i in range(TAPS // 2):
            rows = pl.ds(HEAD + start + c - 2 * i, size, stride=4)
            term = taps[2 * i : 2 * i + 1] * xs[rows, :]
            acc = term if acc is None else acc + term
            acc = acc + taps[2 * i + 1 : 2 * i + 2] * ys[rows, :]
        parts.append(acc)
    return jnp.concatenate(parts, axis=1)


def spectra(ms, frames):
    high, low = split(frames)
    dims = (((1,), (1,)), ((), ()))
    right = jnp.concatenate([high, high], axis=1)
    result = lax.dot_general(ms[...], right, dims, preferred_element_type=jnp.float32)
    return result + lax.dot_general(
        ms[:, 0:256], low, dims, preferred_element_type=jnp.float32
    )


def fine_filter(a1, block, taps, fir):
    for c in range(2):
        for frame in range(32):
            acc = None
            for j in range(min(FINE_TAPS, frame + 1)):
                term = taps(j) * block(c, frame - j)
                acc = term if acc is None else acc + term
            fir[c, pl.ds(8 * frame, 8), :] = acc


def fine_spectra(a1, k, fir, cm, tw):
    rows = []
    for h in range(2):
        parts = [fir[c, pl.ds(2 * k + h, 32, stride=8), :] for c in range(2)]
        rows.append(jnp.concatenate(parts, axis=1))
    high, low = split(jnp.concatenate(rows, axis=0))
    left = jnp.concatenate([high, high, low], axis=1)
    spectrum = jnp.dot(left, cm[...], preferred_element_type=jnp.float32)
    result = []
    for h in range(2):
        a = 2 * a1 + h
        re = spectrum[32 * h : 32 * h + 32, :LANES]
        im = spectrum[32 * h : 32 * h + 32, LANES:]
        if a:
            cos, sin = tw[a : a + 1, :], tw[4 + a : 5 + a, :]
            re, im = re * cos + im * sin, im * cos - re * sin
        result.append((re, im))
    return result


def gather_kernel(
    x_hbm, m_hbm, ct_hbm, ft_hbm, c_hbm, t_hbm, got, extra, taps_out, first, cm, tw,
    xs, ys, ms, ct, ft, ftt, early, tails, heads, sent, fir,
    load_sem, send_sem, recv_sem, ready, again,
):
    loads = [
        pltpu.make_async_copy(ct_hbm, ct, load_sem.at[0]),
        pltpu.make_async_copy(
            x_hbm.at[pl.ds(0, HALF)], xs.at[pl.ds(HEAD, HALF)], load_sem.at[1]
        ),
        pltpu.make_async_copy(
            x_hbm.at[pl.ds(HALF, HALF)], xs.at[pl.ds(HEAD + HALF, HALF)], load_sem.at[2]
        ),
        pltpu.make_async_copy(m_hbm, ms, load_sem.at[3]),
        pltpu.make_async_copy(ft_hbm, ft, load_sem.at[4]),
        pltpu.make_async_copy(c_hbm, cm, load_sem.at[5]),
        pltpu.make_async_copy(t_hbm, tw, load_sem.at[6]),
    ]
    for load in loads[:4]:
        load.start()
    zh, y, c = (lax.axis_index(axis) for axis in TM)
    mine = flat(zh, y, c)
    own = 2 * y + c
    other = 1 - zh
    late = zh == 1
    turn = lax.rem(lax.div(y + 1, 2), 2)
    odd_y = lax.rem(y, 2)
    across = [(dy, dc) for dy in (turn, 1 - turn, 3 - odd_y, 2 + odd_y) for dc in (1, 0)]
    barrier = pltpu.get_barrier_semaphore()
    for at in across:
        pl.semaphore_signal(barrier, inc=1, device_id=named(other, *at), device_id_type=MESH)

    @pl.when(late)
    def _():
        pl.semaphore_wait(barrier, 8)
        for at in across:
            pl.semaphore_signal(
                ready.at[own], inc=1, device_id=named(other, *at), device_id_type=MESH
            )

    xs[pl.ds(0, HEAD), :] = jnp.zeros((HEAD, LANES), jnp.float32)
    xs[pl.ds(HEAD + ROWS, TAIL), :] = jnp.zeros((TAIL, LANES), jnp.float32)
    ys[pl.ds(0, HEAD), :] = jnp.zeros((HEAD, LANES), jnp.float32)
    loads[0].wait()
    taps = ct[...]
    taps = jnp.concatenate([taps, taps], axis=1)

    def delay(start, size):
        left = lax.broadcasted_iota(jnp.int32, (size, LANES), 1) < CHANNELS
        here = xs[pl.ds(start, size), :]
        before = xs[pl.ds(start - 2, size), :]
        ys[pl.ds(start, size), :] = pltpu.roll(jnp.where(left, here, before), CHANNELS, 1)

    def compute(a1, m):
        frames = coarse_frames(xs, ys, taps, HALF * m + 2 * a1, LANES)
        sent[a1, :, :, LANES * m : LANES * (m + 1)] = spectra(ms, frames).reshape(
            PEERS, 16, LANES
        )

    def crossing(piece, source, target):
        return [
            pltpu.make_async_remote_copy(
                src_ref=source.at[flat(other, *at)],
                dst_ref=target.at[mine],
                send_sem=send_sem.at[piece],
                recv_sem=recv_sem.at[piece],
                device_id=named(other, *at),
                device_id_type=MESH,
            )
            for at in across
        ]

    def staying(piece, source, target):
        copies = []
        for dy, dc in BESIDE:
            to = (zh, lax.rem(y + dy, 4), lax.rem(c + dc, 2))
            copy = pltpu.make_async_remote_copy(
                src_ref=source.at[flat(*to)],
                dst_ref=target.at[mine],
                send_sem=send_sem.at[piece],
                recv_sem=recv_sem.at[piece],
                device_id=named(*to),
                device_id_type=MESH,
            )
            copies.append(copy)
        return copies

    def whole(piece, source, target):
        return pltpu.make_async_remote_copy(
            src_ref=source.at[pl.ds(0, 15)],
            dst_ref=target.at[pl.ds(0, 15)],
            send_sem=send_sem.at[piece],
            recv_sem=recv_sem.at[piece],
            device_id=named(other, y, c),
            device_id_type=MESH,
        )

    def part(m, at):
        return pltpu.make_async_remote_copy(
            src_ref=sent.at[0, flat(other, *at), :, pl.ds(LANES * m, LANES)],
            dst_ref=early.at[mine, :, pl.ds(LANES * m, LANES)],
            send_sem=send_sem.at[0],
            recv_sem=recv_sem.at[0],
            device_id=named(other, *at),
            device_id_type=MESH,
        )

    zero = crossing(0, sent.at[0], early)
    one = crossing(1, sent.at[1], got)
    two = crossing(2, tails, heads)

    def start(copies):
        @pl.when(late)
        def _():
            for copy in copies:
                copy.start()

    loads[1].wait()
    delay(HEAD, HALF)
    loads[3].wait()
    compute(0, 0)
    start([part(0, at) for at in across[:4]])
    loads[2].wait()
    delay(HEAD + HALF, HALF + TAIL)
    compute(0, 1)
    start([part(1, at) for at in across[:4]])
    for load in loads[4:]:
        load.start()
    compute(1, 0)
    compute(1, 1)
    start(one[:4])

    ends = [coarse_frames(xs, ys, taps, ROWS + 2 * a1, 8) for a1 in range(2)]
    lower = lax.broadcasted_iota(jnp.int32, (8, 256), 0) < 4
    ends = jnp.where(lower, ends[0], pltpu.roll(ends[1], 4, 0))
    result = spectra(ms, jnp.concatenate([ends] * 16, axis=0))
    chosen = (
        lax.broadcasted_iota(jnp.int32, (16, LANES), 1) // 8
        == lax.broadcasted_iota(jnp.int32, (16, LANES), 0)
    )
    for d in range(PEERS):
        picked = jnp.where(chosen, result[16 * d : 16 * d + 16], 0.0)
        tails[d] = jnp.sum(picked, axis=0, keepdims=True)
    heads[mine] = tails[mine]
    start([*two, *zero[4:], *one[4:]])

    @pl.when(jnp.logical_not(late))
    def _():
        for half in (slice(0, 4), slice(4, 8)):
            for at, copy in zip(across[half], zero[half], strict=True):
                pl.semaphore_wait(ready.at[flat(0, *at)], 1)
                copy.start()
            for copy in (*two[half], *one[half]):
                copy.start()
        pl.semaphore_wait(barrier, 8)
        pl.semaphore_signal(again, inc=1, device_id=named(other, y, c), device_id_type=MESH)

    early[mine] = sent[0, mine]
    got[mine] = sent[1, mine]

    @pl.when(late)
    def _():
        pl.semaphore_wait(again, 1)

    near = [
        *staying(0, sent.at[0], early),
        *staying(2, tails, heads),
        *staying(1, sent.at[1], got),
    ]
    for copy in near:
        copy.start()

    loads[4].wait()
    square = jnp.concatenate([ft[...], jnp.zeros((LANES - FINE_TAPS, FINE), jnp.float32)], axis=0)
    for k in range(4):
        ftt[pl.ds(LANES * k, LANES), :] = square[:, LANES * k : LANES * (k + 1)].T
    by_branch = [ftt[pl.ds(a, LANES, stride=4), :].T for a in range(4)]
    odd = lax.rem(lax.broadcasted_iota(jnp.int32, (8, LANES), 0), 2) == 1
    for a1 in range(2):
        for j in range(FINE_TAPS):
            even_row = jnp.broadcast_to(by_branch[2 * a1][j : j + 1], (8, LANES))
            odd_row = jnp.broadcast_to(by_branch[2 * a1 + 1][j : j + 1], (8, LANES))
            taps_out[a1, j] = jnp.where(odd, odd_row, even_row)
    loads[5].wait()
    loads[6].wait()

    pieces = [whole(0, sent.at[0], early), whole(1, sent.at[1], got), whole(2, tails, heads)]
    pieces[0].wait_recv()
    pieces[2].wait_recv()
    spread = jnp.concatenate(
        [jnp.where(chosen, jnp.broadcast_to(heads[s], (16, LANES)), 0.0) for s in range(PEERS)],
        axis=0,
    )
    row = lax.rem(lax.broadcasted_iota(jnp.int32, (256, 256), 0), 8)
    column = lax.broadcasted_iota(jnp.int32, (256, 256), 1)
    lane = lax.rem(column, LANES)
    select = jnp.logical_and(lane < 4, row == column // LANES * 4 + lane)
    added = jnp.dot(
        jnp.concatenate(split(spread), axis=1),
        jnp.where(select, 1.0, 0.0).astype(jnp.bfloat16),
        preferred_element_type=jnp.float32,
    )
    extra[...] = added[:, LANES:].reshape(PEERS, 16, LANES)

    for s in range(1, PEERS):
        early[s, :, 0:LANES] += added[16 * s - 16 : 16 * s, :LANES]
    fine_filter(
        0,
        lambda c, f: early[f // 2, pl.ds(8 * c, 8), pl.ds(LANES * (f % 2), LANES)],
        lambda j: taps_out[0, j],
        fir,
    )
    for k in range(4):
        for h, parts in enumerate(fine_spectra(0, k, fir, cm, tw)):
            for c in range(2):
                first[k, h, c] = parts[c]

    pieces[0].wait_send()
    pieces[2].wait_send()
    pieces[1].wait()


def fine_kernel(got, extra, taps, first, cm, tw, out, fir, stage, out_sem):
    blocks = {}

    def block(c, frame):
        if (c, frame) not in blocks:
            value = got[frame // 2, pl.ds(8 * c, 8), pl.ds(LANES * (frame % 2), LANES)]
            if frame % 2 == 0 and frame > 0:
                value = value + extra[frame // 2 - 1, pl.ds(8 * c, 8), :]
            blocks[c, frame] = value
        return blocks[c, frame]

    fine_filter(1, block, lambda j: taps[1, j], fir)
    writes = []
    for k in range(4):
        (re1, im1), (re3, im3) = fine_spectra(1, k, fir, cm, tw)
        re0, im0, re2, im2 = first[k, 0, 0], first[k, 0, 1], re1, im1
        re1, im1 = first[k, 1, 0], first[k, 1, 1]
        sum_re, sum_im = re0 + re2, im0 + im2
        dif_re, dif_im = re0 - re2, im0 - im2
        odd_re, odd_im = re1 + re3, im1 + im3
        off_re, off_im = re1 - re3, im1 - im3
        stage[k, 0, :, 0:128] = sum_re + odd_re
        stage[k, 1, :, 0:128] = sum_im + odd_im
        stage[k, 0, :, 128:256] = dif_re + off_im
        stage[k, 1, :, 128:256] = dif_im - off_re
        stage[k, 0, :, 256:384] = sum_re - odd_re
        stage[k, 1, :, 256:384] = sum_im - odd_im
        stage[k, 0, :, 384:512] = dif_re - off_im
        stage[k, 1, :, 384:512] = dif_im + off_re
        for c in range(2):
            write = pltpu.make_async_copy(stage.at[k, c], out.at[c, k], out_sem.at[k, c])
            write.start()
            writes.append(write)
    for write in writes:
        write.wait()


def on_device(signal, coarse_taps, fine_taps):
    rows = signal.reshape(2, HALF, LANES).transpose(1, 0, 2).reshape(ROWS, LANES)
    hbm = pl.BlockSpec(memory_space=pltpu.HBM)
    vmem = pl.BlockSpec(memory_space=pltpu.VMEM)
    tables = [jnp.asarray(v) for v in (coarse_matrix(), fine_matrix(), twiddles())]
    operands = (rows, tables[0], coarse_taps, fine_taps, *tables[1:])
    f32 = jnp.float32
    handed = pl.pallas_call(
        gather_kernel,
        out_shape=[
            jax.ShapeDtypeStruct((PEERS, 16, 256), f32),
            jax.ShapeDtypeStruct((PEERS, 16, LANES), f32),
            jax.ShapeDtypeStruct((2, FINE_TAPS, 8, LANES), f32),
            jax.ShapeDtypeStruct((4, 2, 2, 32, LANES), f32),
            jax.ShapeDtypeStruct((768, 256), jnp.bfloat16),
            jax.ShapeDtypeStruct((8, LANES), f32),
        ],
        in_specs=[hbm] * 6,
        out_specs=[vmem] * 6,
        scratch_shapes=[
            pltpu.VMEM((HEAD + ROWS + TAIL, LANES), f32),
            pltpu.VMEM((HEAD + ROWS + TAIL, LANES), f32),
            pltpu.VMEM((256, 512), jnp.bfloat16),
            pltpu.VMEM((TAPS, CHANNELS), f32),
            pltpu.VMEM((FINE_TAPS, FINE), f32),
            pltpu.VMEM((FINE, LANES), f32),
            pltpu.VMEM((PEERS, 16, 256), f32),
            pltpu.VMEM((PEERS, 1, LANES), f32),
            pltpu.VMEM((PEERS, 1, LANES), f32),
            pltpu.VMEM((2, PEERS, 16, 256), f32),
            pltpu.VMEM((2, 256, LANES), f32),
            pltpu.SemaphoreType.DMA((7,)),
            pltpu.SemaphoreType.DMA((3,)),
            pltpu.SemaphoreType.DMA((3,)),
            pltpu.SemaphoreType.REGULAR((8,)),
            pltpu.SemaphoreType.REGULAR,
        ],
        compiler_params=pltpu.CompilerParams(
            collective_id=0, has_side_effects=True, vmem_limit_bytes=16 << 20
        ),
        name="gather",
    )(*(pltpu.with_memory_space_constraint(v, pltpu.HBM) for v in operands))
    return pl.pallas_call(
        fine_kernel,
        out_shape=jax.ShapeDtypeStruct((2, 4, 32, FINE), f32),
        in_specs=[vmem] * 6,
        out_specs=hbm,
        scratch_shapes=[
            pltpu.VMEM((2, 256, LANES), f32),
            pltpu.VMEM((4, 2, 32, FINE), f32),
            pltpu.SemaphoreType.DMA((4, 2)),
        ],
        compiler_params=pltpu.CompilerParams(vmem_limit_bytes=16 << 20),
        name="fine",
    )(*handed)


def solution(mesh):
    finer = Mesh(mesh.devices.reshape(mesh.shape["streams"], *GROUP), ("streams", *TM))
    return jax.shard_map(
        on_device,
        mesh=finer,
        in_specs=(P(None, ("streams", *TM)), P(), P()),
        out_specs=P(None, TM, "streams", None),
        check_vma=False,
    )
```

```python
import functools
import math

import jax
import jax.numpy as jnp
import numpy as np
from jax import lax
from jax.experimental import pallas as pl
from jax.experimental.pallas import tpu as pltpu
from jax.sharding import Mesh
from jax.sharding import PartitionSpec as P

CHANNELS = 64
FINE = 512
TAPS = 16
FINE_TAPS = 12
TM = ("zh", "y", "c")
GROUP = (2, 4, 2)
PEERS = 16
LANES = 128
HEAD = 16
TAIL = 32
ROWS = 1024
HALF = 512
MESH = pl.DeviceIdType.MESH
BESIDE = [(dy, dc) for dy in (2, 1, 3, 0) for dc in (1, 0) if (dy, dc) != (0, 0)]


def split(value):
    high = value.astype(jnp.bfloat16)
    low = (value - high.astype(jnp.float32)).astype(jnp.bfloat16)
    return high, low


def np_split(value):
    value = value.astype(np.float32)
    high = value.astype(jnp.bfloat16)
    low = (value - high.astype(np.float32)).astype(jnp.bfloat16)
    return high, low


def coarse_matrix():
    owner, part, own, parity = np.meshgrid(
        np.arange(16), np.arange(2), np.arange(4), np.arange(2), indexing="ij"
    )
    channel = (4 * owner + own).reshape(-1, 1)
    part, parity = part.reshape(-1, 1), parity.reshape(-1, 1)
    part_in, parity_in, branch = np.meshgrid(
        np.arange(2), np.arange(2), np.arange(CHANNELS), indexing="ij"
    )
    part_in, parity_in, branch = (v.reshape(1, -1) for v in (part_in, parity_in, branch))
    angle = 2.0 * np.pi * (channel * branch % CHANNELS) / CHANNELS
    value = np.where(part == part_in, np.cos(angle), np.sin(angle) * (part_in - part))
    value = np.where(parity == parity_in, value, 0.0) / math.sqrt(CHANNELS)
    return np.concatenate(np_split(value), axis=1)


def fine_matrix():
    part_in, b = np.meshgrid(np.arange(2), np.arange(LANES), indexing="ij")
    part_in, b = part_in.reshape(-1, 1), b.reshape(-1, 1)
    part, c = part_in.reshape(1, -1), b.reshape(1, -1)
    angle = 2.0 * np.pi * (b * c % LANES) / LANES
    value = np.where(part == part_in, np.cos(angle), np.sin(angle) * (part_in - part))
    high, low = np_split(value / math.sqrt(FINE))
    return np.concatenate([high, low, high], axis=0)


def twiddles():
    a, c = np.meshgrid(np.arange(4), np.arange(LANES), indexing="ij")
    angle = 2.0 * np.pi * a * c / FINE
    return np.concatenate([np.cos(angle), np.sin(angle)]).astype(np.float32)


def flat(zh, y, c):
    return (zh * 4 + y) * 2 + c


def named(zh, y, c):
    return {"zh": zh, "y": y, "c": c}


def coarse_frames(xs, ys, taps, start, size):
    parts = []
    for c in range(2):
        acc = None
        for i in range(TAPS // 2):
            rows = pl.ds(HEAD + start + c - 2 * i, size, stride=4)
            term = taps[2 * i : 2 * i + 1] * xs[rows, :]
            acc = term if acc is None else acc + term
            acc = acc + taps[2 * i + 1 : 2 * i + 2] * ys[rows, :]
        parts.append(acc)
    return jnp.concatenate(parts, axis=1)


def spectra(ms, frames):
    high, low = split(frames)
    dims = (((1,), (1,)), ((), ()))
    right = jnp.concatenate([high, high], axis=1)
    result = lax.dot_general(ms[...], right, dims, preferred_element_type=jnp.float32)
    return result + lax.dot_general(
        ms[:, 0:256], low, dims, preferred_element_type=jnp.float32
    )


def fine_filter(half, block, taps, fir):
    for c in range(2):
        blocks = {}
        for frame in range(16 * half, 16 * half + 16):
            acc = None
            for j in range(min(FINE_TAPS, frame + 1)):
                at = frame - j
                if at not in blocks:
                    blocks[at] = block(c, at)
                term = taps(j) * blocks[at]
                acc = term if acc is None else acc + term
            fir[c, pl.ds(8 * (frame - 16 * half), 8), :] = acc


def fine_spectra(a1, fir, cm, tw):
    rows = []
    for h in range(2):
        for k in range(4):
            parts = [fir[c, pl.ds(2 * k + h, 16, stride=8), :] for c in range(2)]
            rows.append(jnp.concatenate(parts, axis=1))
    high, low = split(jnp.concatenate(rows, axis=0))
    left = jnp.concatenate([high, high, low], axis=1)
    spectrum = jnp.dot(left, cm[...], preferred_element_type=jnp.float32)
    result = []
    for h in range(2):
        a = 2 * a1 + h
        re = spectrum[64 * h : 64 * h + 64, :LANES]
        im = spectrum[64 * h : 64 * h + 64, LANES:]
        if a:
            cos, sin = tw[a : a + 1, :], tw[4 + a : 5 + a, :]
            re, im = re * cos + im * sin, im * cos - re * sin
        result.append((re, im))
    (re0, im0), (re1, im1) = result
    quarters = [
        (re0 + re1, im0 + im1),
        (re0 + im1, im0 - re1),
        (re0 - re1, im0 - im1),
        (re0 - im1, im0 + re1),
    ]
    if a1:
        quarters = [(-re, -im) if d % 2 else (re, im) for d, (re, im) in enumerate(quarters)]
    return quarters


def classes(a1, half, blocks, over_end, taps, fir, cm, tw):
    def block(c, frame):
        value = blocks[frame // 2, pl.ds(8 * c, 8), pl.ds(LANES * (frame % 2), LANES)]
        if frame % 2 == 0 and frame > 0:
            value = value + over_end[frame // 2 - 1, pl.ds(8 * c, 8), :]
        return value

    fine_filter(half, block, lambda j: taps[a1, j], fir)
    return fine_spectra(a1, fir, cm, tw)


def gather_kernel(
    x_hbm, m_hbm, ct_hbm, ft_hbm, c_hbm, t_hbm, got, extra, taps_out, first, cm, tw,
    xs, ys, ms, ct, ft, ftt, early, tails, heads, sent, over_end, fir,
    load_sem, send_sem, recv_sem, ready, again,
):
    loads = [
        pltpu.make_async_copy(ct_hbm, ct, load_sem.at[0]),
        pltpu.make_async_copy(
            x_hbm.at[pl.ds(0, HALF)], xs.at[pl.ds(HEAD, HALF)], load_sem.at[1]
        ),
        pltpu.make_async_copy(
            x_hbm.at[pl.ds(HALF, HALF)], xs.at[pl.ds(HEAD + HALF, HALF)], load_sem.at[2]
        ),
        pltpu.make_async_copy(m_hbm, ms, load_sem.at[3]),
        pltpu.make_async_copy(ft_hbm, ft, load_sem.at[4]),
        pltpu.make_async_copy(c_hbm, cm, load_sem.at[5]),
        pltpu.make_async_copy(t_hbm, tw, load_sem.at[6]),
    ]
    for load in loads[:4]:
        load.start()
    zh, y, c = (lax.axis_index(axis) for axis in TM)
    mine = flat(zh, y, c)
    own = 2 * y + c
    other = 1 - zh
    late = zh == 1
    patient = jnp.logical_and(zh == 0, lax.div(lax.axis_index("streams"), 4) == 1)
    turn = lax.rem(lax.div(y + 1, 2), 2)
    odd_y = lax.rem(y, 2)
    across = [(dy, dc) for dy in (turn, 1 - turn, 3 - odd_y, 2 + odd_y) for dc in (1, 0)]
    barrier = pltpu.get_barrier_semaphore()
    for at in across:
        pl.semaphore_signal(barrier, inc=1, device_id=named(other, *at), device_id_type=MESH)

    @pl.when(late)
    def _():
        pl.semaphore_wait(barrier, 8)
        for at in across:
            pl.semaphore_signal(
                ready.at[own], inc=1, device_id=named(other, *at), device_id_type=MESH
            )

    xs[pl.ds(0, HEAD), :] = jnp.zeros((HEAD, LANES), jnp.float32)
    xs[pl.ds(HEAD + ROWS, TAIL), :] = jnp.zeros((TAIL, LANES), jnp.float32)
    ys[pl.ds(0, HEAD), :] = jnp.zeros((HEAD, LANES), jnp.float32)
    loads[0].wait()
    taps = ct[...]
    taps = jnp.concatenate([taps, taps], axis=1)

    def delay(start, size):
        left = lax.broadcasted_iota(jnp.int32, (size, LANES), 1) < CHANNELS
        here = xs[pl.ds(start, size), :]
        before = xs[pl.ds(start - 2, size), :]
        ys[pl.ds(start, size), :] = pltpu.roll(jnp.where(left, here, before), CHANNELS, 1)

    def compute(a1, m):
        frames = coarse_frames(xs, ys, taps, HALF * m + 2 * a1, LANES)
        sent[a1, :, :, LANES * m : LANES * (m + 1)] = spectra(ms, frames).reshape(
            PEERS, 16, LANES
        )

    def prepare():
        loads[4].wait()
        square = jnp.concatenate([ft[...], jnp.zeros((LANES - FINE_TAPS, FINE), jnp.float32)], axis=0)
        for k in range(4):
            ftt[pl.ds(LANES * k, LANES), :] = square[:, LANES * k : LANES * (k + 1)].T
        by_branch = [ftt[pl.ds(a, LANES, stride=4), :].T for a in range(4)]
        odd = lax.rem(lax.broadcasted_iota(jnp.int32, (8, LANES), 0), 2) == 1
        for a1 in range(2):
            for j in range(FINE_TAPS):
                even_row = jnp.broadcast_to(by_branch[2 * a1][j : j + 1], (8, LANES))
                odd_row = jnp.broadcast_to(by_branch[2 * a1 + 1][j : j + 1], (8, LANES))
                taps_out[a1, j] = jnp.where(odd, odd_row, even_row)

    def crossing(piece, source, target):
        return [
            pltpu.make_async_remote_copy(
                src_ref=source.at[flat(other, *at)],
                dst_ref=target.at[mine],
                send_sem=send_sem.at[piece],
                recv_sem=recv_sem.at[piece],
                device_id=named(other, *at),
                device_id_type=MESH,
            )
            for at in across
        ]

    def staying(piece, source, target):
        copies = []
        for dy, dc in BESIDE:
            to = (zh, lax.rem(y + dy, 4), lax.rem(c + dc, 2))
            copy = pltpu.make_async_remote_copy(
                src_ref=source.at[flat(*to)],
                dst_ref=target.at[mine],
                send_sem=send_sem.at[piece],
                recv_sem=recv_sem.at[piece + 3],
                device_id=named(*to),
                device_id_type=MESH,
            )
            copies.append(copy)
        return copies

    def whole(piece, target, count, near):
        return pltpu.make_async_remote_copy(
            src_ref=target.at[pl.ds(0, count)],
            dst_ref=target.at[pl.ds(0, count)],
            send_sem=send_sem.at[piece],
            recv_sem=recv_sem.at[piece + 3 * near],
            device_id=named(other, y, c),
            device_id_type=MESH,
        )

    def part(m, at):
        return pltpu.make_async_remote_copy(
            src_ref=sent.at[0, flat(other, *at), :, pl.ds(LANES * m, LANES)],
            dst_ref=early.at[mine, :, pl.ds(LANES * m, LANES)],
            send_sem=send_sem.at[0],
            recv_sem=recv_sem.at[0],
            device_id=named(other, *at),
            device_id_type=MESH,
        )

    zero = crossing(0, sent.at[0], early)
    one = crossing(1, sent.at[1], got)
    two = crossing(2, tails, heads)

    def start(copies):
        @pl.when(late)
        def _():
            for copy in copies:
                copy.start()

    loads[1].wait()
    delay(HEAD, HALF)
    loads[3].wait()
    compute(0, 0)
    start([part(0, at) for at in across[:4]])
    loads[2].wait()
    delay(HEAD + HALF, HALF + TAIL)
    compute(0, 1)
    start([part(1, at) for at in across[:4]])
    for load in loads[4:]:
        load.start()
    compute(1, 0)
    compute(1, 1)
    start(one[:4])

    ends = [coarse_frames(xs, ys, taps, ROWS + 2 * a1, 8) for a1 in range(2)]
    lower = lax.broadcasted_iota(jnp.int32, (8, 256), 0) < 4
    ends = jnp.where(lower, ends[0], pltpu.roll(ends[1], 4, 0))
    result = spectra(ms, jnp.concatenate([ends] * 16, axis=0))
    chosen = (
        lax.broadcasted_iota(jnp.int32, (16, LANES), 1) // 8
        == lax.broadcasted_iota(jnp.int32, (16, LANES), 0)
    )
    for d in range(PEERS):
        picked = jnp.where(chosen, result[16 * d : 16 * d + 16], 0.0)
        tails[d] = jnp.sum(picked, axis=0, keepdims=True)
    heads[mine] = tails[mine]
    start([*two, *zero[4:], *one[4:]])

    @pl.when(jnp.logical_not(late))
    def _():
        @pl.when(patient)
        def _():
            pl.semaphore_wait(barrier, 8)
            prepare()

        for half in (slice(0, 4), slice(4, 8)):
            for at, copy in zip(across[half], zero[half], strict=True):
                pl.semaphore_wait(ready.at[flat(0, *at)], 1)
                copy.start()
            for copy in (*two[half], *one[half]):
                copy.start()
        @pl.when(jnp.logical_not(patient))
        def _():
            pl.semaphore_wait(barrier, 8)

        pl.semaphore_signal(again, inc=1, device_id=named(other, y, c), device_id_type=MESH)

    early[mine] = sent[0, mine]
    got[mine] = sent[1, mine]

    @pl.when(late)
    def _():
        pl.semaphore_wait(again, 1)

    near = [
        *staying(0, sent.at[0], early),
        *staying(2, tails, heads),
        *staying(1, sent.at[1], got),
    ]
    for copy in near:
        copy.start()

    @pl.when(jnp.logical_not(patient))
    def _():
        prepare()

    loads[5].wait()
    loads[6].wait()

    def wait_for(count, near):
        whole(0, early, count, near).wait_recv()
        whole(2, heads, count, near).wait_recv()

    row = lax.rem(lax.broadcasted_iota(jnp.int32, (256, 256), 0), 8)
    column = lax.broadcasted_iota(jnp.int32, (256, 256), 1)
    lane = lax.rem(column, LANES)
    select = jnp.logical_and(lane < 4, row == column // LANES * 4 + lane)
    select = jnp.where(select, 1.0, 0.0).astype(jnp.bfloat16)

    def spread(half):
        some = slice(8 * half, 8 * half + 8)
        picked = [
            jnp.where(chosen, jnp.broadcast_to(heads[s], (16, LANES)), 0.0)
            for s in range(8 * half, 8 * half + 8)
        ]
        added = jnp.dot(
            jnp.concatenate(split(jnp.concatenate(picked, axis=0)), axis=1),
            select,
            preferred_element_type=jnp.float32,
        ).reshape(8, 16, 256)
        over_end[some] = added[:, :, :LANES]
        extra[some] = added[:, :, LANES:]

    def put(half, quarters, add):
        rows = slice(16 * half, 16 * half + 16)
        for d, both in enumerate(quarters):
            lanes = slice(LANES * d, LANES * d + LANES)
            for part, value in enumerate(both):
                value = value.reshape(4, 16, LANES)
                if add:
                    value = value + first[part, :, rows, lanes]
                first[part, :, rows, lanes] = value

    wait_for(7, True)
    whole(1, got, 7, True).wait_recv()

    @pl.when(late)
    def _():
        wait_for(8, False)

    spread(0)
    put(0, classes(0, 0, early, over_end, taps_out, fir, cm, tw), False)

    @pl.when(jnp.logical_not(late))
    def _():
        put(0, classes(1, 0, got, extra, taps_out, fir, cm, tw), True)
        wait_for(8, False)

    spread(1)
    put(1, classes(0, 1, early, over_end, taps_out, fir, cm, tw), False)
    whole(0, early, 15, True).wait_send()
    whole(2, heads, 15, True).wait_send()
    whole(1, got, 8, False).wait_recv()
    whole(1, got, 15, True).wait_send()


def fine_kernel(got, extra, taps, first, cm, tw, out, fir, stage, out_sem):
    late = lax.axis_index("zh") == 1

    def write(source, half, k):
        rows = pl.ds(16 * half, 16)
        return pltpu.make_async_copy(
            source.at[:, k, rows], out.at[:, k, rows], out_sem.at[half, k]
        )

    def finish(half):
        rows = slice(16 * half, 16 * half + 16)
        quarters = classes(1, half, got, extra, taps, fir, cm, tw)
        for k in range(4):
            for d, both in enumerate(quarters):
                lanes = slice(LANES * d, LANES * d + LANES)
                for part, value in enumerate(both):
                    stage[part, k, rows, lanes] = (
                        first[part, k, rows, lanes] + value[16 * k : 16 * k + 16]
                    )
            write(stage, half, k).start()

    @pl.when(jnp.logical_not(late))
    def _():
        for k in range(4):
            write(first, 0, k).start()

    @pl.when(late)
    def _():
        finish(0)

    finish(1)
    for half in range(2):
        for k in range(4):
            write(stage, half, k).wait()


def on_device(signal, coarse_taps, fine_taps):
    rows = signal.reshape(2, HALF, LANES).transpose(1, 0, 2).reshape(ROWS, LANES)
    hbm = pl.BlockSpec(memory_space=pltpu.HBM)
    vmem = pl.BlockSpec(memory_space=pltpu.VMEM)
    tables = [jnp.asarray(v) for v in (coarse_matrix(), fine_matrix(), twiddles())]
    operands = (rows, tables[0], coarse_taps, fine_taps, *tables[1:])
    f32 = jnp.float32
    handed = pl.pallas_call(
        gather_kernel,
        out_shape=[
            jax.ShapeDtypeStruct((PEERS, 16, 256), f32),
            jax.ShapeDtypeStruct((PEERS, 16, LANES), f32),
            jax.ShapeDtypeStruct((2, FINE_TAPS, 8, LANES), f32),
            jax.ShapeDtypeStruct((2, 4, 32, FINE), f32),
            jax.ShapeDtypeStruct((768, 256), jnp.bfloat16),
            jax.ShapeDtypeStruct((8, LANES), f32),
        ],
        in_specs=[hbm] * 6,
        out_specs=[vmem] * 6,
        scratch_shapes=[
            pltpu.VMEM((HEAD + ROWS + TAIL, LANES), f32),
            pltpu.VMEM((HEAD + ROWS + TAIL, LANES), f32),
            pltpu.VMEM((256, 512), jnp.bfloat16),
            pltpu.VMEM((TAPS, CHANNELS), f32),
            pltpu.VMEM((FINE_TAPS, FINE), f32),
            pltpu.VMEM((FINE, LANES), f32),
            pltpu.VMEM((PEERS, 16, 256), f32),
            pltpu.VMEM((PEERS, 1, LANES), f32),
            pltpu.VMEM((PEERS, 1, LANES), f32),
            pltpu.VMEM((2, PEERS, 16, 256), f32),
            pltpu.VMEM((PEERS, 16, LANES), f32),
            pltpu.VMEM((2, LANES, LANES), f32),
            pltpu.SemaphoreType.DMA((7,)),
            pltpu.SemaphoreType.DMA((3,)),
            pltpu.SemaphoreType.DMA((6,)),
            pltpu.SemaphoreType.REGULAR((8,)),
            pltpu.SemaphoreType.REGULAR,
        ],
        compiler_params=pltpu.CompilerParams(
            collective_id=0, has_side_effects=True, vmem_limit_bytes=16 << 20
        ),
        name="gather",
    )(*(pltpu.with_memory_space_constraint(v, pltpu.HBM) for v in operands))
    return pl.pallas_call(
        fine_kernel,
        out_shape=jax.ShapeDtypeStruct((2, 4, 32, FINE), f32),
        in_specs=[vmem] * 6,
        out_specs=hbm,
        scratch_shapes=[
            pltpu.VMEM((2, LANES, LANES), f32),
            pltpu.VMEM((2, 4, 32, FINE), f32),
            pltpu.SemaphoreType.DMA((2, 4)),
        ],
        compiler_params=pltpu.CompilerParams(vmem_limit_bytes=16 << 20),
        name="fine",
    )(*handed)


def solution(mesh):
    finer = Mesh(mesh.devices.reshape(mesh.shape["streams"], *GROUP), ("streams", *TM))
    return jax.shard_map(
        on_device,
        mesh=finer,
        in_specs=(P(None, ("streams", *TM)), P(), P()),
        out_specs=P(None, TM, "streams", None),
        check_vma=False,
    )
```

```python
import functools
import math

import jax
import jax.numpy as jnp
import numpy as np
from jax import lax
from jax.experimental import pallas as pl
from jax.experimental.pallas import tpu as pltpu
from jax.sharding import Mesh
from jax.sharding import PartitionSpec as P

CHANNELS = 64
FINE = 512
TAPS = 16
FINE_TAPS = 12
TM = ("zh", "y", "c")
GROUP = (2, 4, 2)
PEERS = 16
LANES = 128
HEAD = 16
TAIL = 32
ROWS = 1024
HALF = 512
MESH = pl.DeviceIdType.MESH
BESIDE = [(dy, dc) for dy in (2, 1, 3, 0) for dc in (1, 0) if (dy, dc) != (0, 0)]


def split(value):
    high = value.astype(jnp.bfloat16)
    low = (value - high.astype(jnp.float32)).astype(jnp.bfloat16)
    return high, low


def np_split(value):
    value = value.astype(np.float32)
    high = value.astype(jnp.bfloat16)
    low = (value - high.astype(np.float32)).astype(jnp.bfloat16)
    return high, low


def coarse_matrix():
    owner, part, own, parity = np.meshgrid(
        np.arange(16), np.arange(2), np.arange(4), np.arange(2), indexing="ij"
    )
    channel = (4 * owner + own).reshape(-1, 1)
    part, parity = part.reshape(-1, 1), parity.reshape(-1, 1)
    part_in, parity_in, branch = np.meshgrid(
        np.arange(2), np.arange(2), np.arange(CHANNELS), indexing="ij"
    )
    part_in, parity_in, branch = (v.reshape(1, -1) for v in (part_in, parity_in, branch))
    angle = 2.0 * np.pi * (channel * branch % CHANNELS) / CHANNELS
    value = np.where(part == part_in, np.cos(angle), np.sin(angle) * (part_in - part))
    value = np.where(parity == parity_in, value, 0.0) / math.sqrt(CHANNELS)
    return np.concatenate(np_split(value), axis=1)


def fine_matrix():
    part_in, b = np.meshgrid(np.arange(2), np.arange(LANES), indexing="ij")
    part_in, b = part_in.reshape(-1, 1), b.reshape(-1, 1)
    part, c = part_in.reshape(1, -1), b.reshape(1, -1)
    angle = 2.0 * np.pi * (b * c % LANES) / LANES
    value = np.where(part == part_in, np.cos(angle), np.sin(angle) * (part_in - part))
    high, low = np_split(value / math.sqrt(FINE))
    return np.concatenate([high, low, high], axis=0)


def twiddles():
    a, c = np.meshgrid(np.arange(4), np.arange(LANES), indexing="ij")
    angle = 2.0 * np.pi * a * c / FINE
    return np.concatenate([np.cos(angle), np.sin(angle)]).astype(np.float32)


def flat(zh, y, c):
    return (zh * 4 + y) * 2 + c


def named(zh, y, c):
    return {"zh": zh, "y": y, "c": c}


def coarse_frames(xs, ys, taps, start, size):
    parts = []
    for c in range(2):
        acc = None
        for i in range(TAPS // 2):
            rows = pl.ds(HEAD + start + c - 2 * i, size, stride=4)
            term = taps[2 * i : 2 * i + 1] * xs[rows, :]
            acc = term if acc is None else acc + term
            acc = acc + taps[2 * i + 1 : 2 * i + 2] * ys[rows, :]
        parts.append(acc)
    return jnp.concatenate(parts, axis=1)


def spectra(ms, frames):
    high, low = split(frames)
    dims = (((1,), (1,)), ((), ()))
    right = jnp.concatenate([high, high], axis=1)
    result = lax.dot_general(ms[...], right, dims, preferred_element_type=jnp.float32)
    return result + lax.dot_general(
        ms[:, 0:256], low, dims, preferred_element_type=jnp.float32
    )


def fine_filter(start, count, block, taps, fir):
    for c in range(2):
        blocks = {}
        for frame in range(start, start + count):
            acc = None
            for j in range(min(FINE_TAPS, frame + 1)):
                at = frame - j
                if at not in blocks:
                    blocks[at] = block(c, at)
                term = taps(j) * blocks[at]
                acc = term if acc is None else acc + term
            fir[c, pl.ds(8 * (frame - start), 8), :] = acc


def fine_spectra(a1, count, fir, cm, tw):
    rows = []
    for h in range(2):
        for k in range(4):
            parts = [fir[c, pl.ds(2 * k + h, count, stride=8), :] for c in range(2)]
            rows.append(jnp.concatenate(parts, axis=1))
    high, low = split(jnp.concatenate(rows, axis=0))
    left = jnp.concatenate([high, high, low], axis=1)
    spectrum = jnp.dot(left, cm[...], preferred_element_type=jnp.float32)
    result = []
    for h in range(2):
        a = 2 * a1 + h
        rows = slice(4 * count * h, 4 * count * (h + 1))
        re, im = spectrum[rows, :LANES], spectrum[rows, LANES:]
        if a:
            cos, sin = tw[a : a + 1, :], tw[4 + a : 5 + a, :]
            re, im = re * cos + im * sin, im * cos - re * sin
        result.append((re, im))
    (re0, im0), (re1, im1) = result
    quarters = [
        (re0 + re1, im0 + im1),
        (re0 + im1, im0 - re1),
        (re0 - re1, im0 - im1),
        (re0 - im1, im0 + re1),
    ]
    if a1:
        quarters = [(-re, -im) if d % 2 else (re, im) for d, (re, im) in enumerate(quarters)]
    return quarters


def classes(a1, start, count, blocks, over_end, taps, fir, cm, tw):
    def block(c, frame):
        value = blocks[frame // 2, pl.ds(8 * c, 8), pl.ds(LANES * (frame % 2), LANES)]
        if frame % 2 == 0 and frame > 0:
            value = value + over_end[frame // 2 - 1, pl.ds(8 * c, 8), :]
        return value

    fine_filter(start, count, block, lambda j: taps[a1, j], fir)
    return fine_spectra(a1, count, fir, cm, tw)


def gather_kernel(
    x_hbm, m_hbm, ct_hbm, ft_hbm, c_hbm, t_hbm, got, extra, taps_out, first, cm, tw,
    xs, ys, ms, ct, ft, ftt, early, tails, heads, sent, over_end, fir,
    load_sem, send_sem, recv_sem, ready, again,
):
    loads = [
        pltpu.make_async_copy(ct_hbm, ct, load_sem.at[0]),
        pltpu.make_async_copy(
            x_hbm.at[pl.ds(0, HALF)], xs.at[pl.ds(HEAD, HALF)], load_sem.at[1]
        ),
        pltpu.make_async_copy(
            x_hbm.at[pl.ds(HALF, HALF)], xs.at[pl.ds(HEAD + HALF, HALF)], load_sem.at[2]
        ),
        pltpu.make_async_copy(m_hbm, ms, load_sem.at[3]),
        pltpu.make_async_copy(ft_hbm, ft, load_sem.at[4]),
        pltpu.make_async_copy(c_hbm, cm, load_sem.at[5]),
        pltpu.make_async_copy(t_hbm, tw, load_sem.at[6]),
    ]
    for load in loads[:4]:
        load.start()
    zh, y, c = (lax.axis_index(axis) for axis in TM)
    mine = flat(zh, y, c)
    own = 2 * y + c
    other = 1 - zh
    late = zh == 1
    patient = jnp.logical_and(zh == 0, lax.div(lax.axis_index("streams"), 4) == 1)
    turn = lax.rem(lax.div(y + 1, 2), 2)
    def pick(*table):
        by_y = [jnp.where(y == 2, t[2], t[3]) for t in zip(*table, strict=True)]
        by_y = [jnp.where(y == 1, t[1], v) for t, v in zip(zip(*table), by_y, strict=True)]
        return [jnp.where(y == 0, t[0], v) for t, v in zip(zip(*table), by_y, strict=True)]

    to_early = pick((2, 1, 0, 3), (3, 0, 1, 2), (0, 1, 3, 2), (1, 0, 2, 3))
    to_late = [turn, 1 - turn, 2 + turn, 3 - turn]
    order = [jnp.where(late, p, q) for p, q in zip(to_early, to_late, strict=True)]
    across = [(dy, dc) for dy in order for dc in (1, 0)]
    barrier = pltpu.get_barrier_semaphore()
    for at in across:
        pl.semaphore_signal(barrier, inc=1, device_id=named(other, *at), device_id_type=MESH)

    @pl.when(late)
    def _():
        pl.semaphore_wait(barrier, 8)
        for at in across:
            pl.semaphore_signal(
                ready.at[own], inc=1, device_id=named(other, *at), device_id_type=MESH
            )

    xs[pl.ds(0, HEAD), :] = jnp.zeros((HEAD, LANES), jnp.float32)
    xs[pl.ds(HEAD + ROWS, TAIL), :] = jnp.zeros((TAIL, LANES), jnp.float32)
    ys[pl.ds(0, HEAD), :] = jnp.zeros((HEAD, LANES), jnp.float32)
    loads[0].wait()
    taps = ct[...]
    taps = jnp.concatenate([taps, taps], axis=1)

    def delay(start, size):
        left = lax.broadcasted_iota(jnp.int32, (size, LANES), 1) < CHANNELS
        here = xs[pl.ds(start, size), :]
        before = xs[pl.ds(start - 2, size), :]
        ys[pl.ds(start, size), :] = pltpu.roll(jnp.where(left, here, before), CHANNELS, 1)

    def compute(a1, m):
        frames = coarse_frames(xs, ys, taps, HALF * m + 2 * a1, LANES)
        sent[a1, :, :, LANES * m : LANES * (m + 1)] = spectra(ms, frames).reshape(
            PEERS, 16, LANES
        )

    def turned():
        loads[4].wait()
        square = jnp.concatenate(
            [ft[...], jnp.zeros((LANES - FINE_TAPS, FINE), jnp.float32)], axis=0
        )
        for k in range(4):
            ftt[pl.ds(LANES * k, LANES), :] = square[:, LANES * k : LANES * (k + 1)].T

    def sorted_taps():
        by_branch = [ftt[pl.ds(a, LANES, stride=4), :].T for a in range(4)]
        odd = lax.rem(lax.broadcasted_iota(jnp.int32, (8, LANES), 0), 2) == 1
        for a1 in range(2):
            for j in range(FINE_TAPS):
                even_row = jnp.broadcast_to(by_branch[2 * a1][j : j + 1], (8, LANES))
                odd_row = jnp.broadcast_to(by_branch[2 * a1 + 1][j : j + 1], (8, LANES))
                taps_out[a1, j] = jnp.where(odd, odd_row, even_row)

    def crossing(piece, source, target):
        return [
            pltpu.make_async_remote_copy(
                src_ref=source.at[flat(other, *at)],
                dst_ref=target.at[mine],
                send_sem=send_sem.at[piece],
                recv_sem=recv_sem.at[piece],
                device_id=named(other, *at),
                device_id_type=MESH,
            )
            for at in across
        ]

    def staying(piece, source, target):
        copies = []
        for dy, dc in BESIDE:
            to = (zh, lax.rem(y + dy, 4), lax.rem(c + dc, 2))
            copy = pltpu.make_async_remote_copy(
                src_ref=source.at[flat(*to)],
                dst_ref=target.at[mine],
                send_sem=send_sem.at[piece],
                recv_sem=recv_sem.at[piece + 3],
                device_id=named(*to),
                device_id_type=MESH,
            )
            copies.append(copy)
        return copies

    def whole(piece, target, count, near):
        return pltpu.make_async_remote_copy(
            src_ref=target.at[pl.ds(0, count)],
            dst_ref=target.at[pl.ds(0, count)],
            send_sem=send_sem.at[piece],
            recv_sem=recv_sem.at[piece + 3 * near],
            device_id=named(other, y, c),
            device_id_type=MESH,
        )

    def part(m, at):
        return pltpu.make_async_remote_copy(
            src_ref=sent.at[0, flat(other, *at), :, pl.ds(LANES * m, LANES)],
            dst_ref=early.at[mine, :, pl.ds(LANES * m, LANES)],
            send_sem=send_sem.at[0],
            recv_sem=recv_sem.at[0],
            device_id=named(other, *at),
            device_id_type=MESH,
        )

    zero = crossing(0, sent.at[0], early)
    one = crossing(1, sent.at[1], got)
    two = crossing(2, tails, heads)

    def start(copies):
        @pl.when(late)
        def _():
            for copy in copies:
                copy.start()

    loads[1].wait()
    delay(HEAD, HALF)
    loads[3].wait()
    compute(0, 0)
    start([part(0, at) for at in across[:4]])
    loads[2].wait()
    delay(HEAD + HALF, HALF + TAIL)
    compute(0, 1)
    start([part(1, at) for at in across[:4]])
    for load in loads[4:]:
        load.start()
    compute(1, 0)
    compute(1, 1)
    start(one[:4])

    ends = [coarse_frames(xs, ys, taps, ROWS + 2 * a1, 8) for a1 in range(2)]
    lower = lax.broadcasted_iota(jnp.int32, (8, 256), 0) < 4
    ends = jnp.where(lower, ends[0], pltpu.roll(ends[1], 4, 0))
    result = spectra(ms, jnp.concatenate([ends] * 16, axis=0))
    chosen = (
        lax.broadcasted_iota(jnp.int32, (16, LANES), 1) // 8
        == lax.broadcasted_iota(jnp.int32, (16, LANES), 0)
    )
    for d in range(PEERS):
        picked = jnp.where(chosen, result[16 * d : 16 * d + 16], 0.0)
        tails[d] = jnp.sum(picked, axis=0, keepdims=True)
    heads[mine] = tails[mine]
    start([*two, *zero[4:], *one[4:]])

    @pl.when(jnp.logical_not(late))
    def _():
        @pl.when(patient)
        def _():
            pl.semaphore_wait(barrier, 8)
            turned()

        for half in (slice(0, 4), slice(4, 8)):
            for at, copy in zip(across[half], zero[half], strict=True):
                pl.semaphore_wait(ready.at[flat(0, *at)], 1)
                copy.start()
            for copy in (*two[half], *one[half]):
                copy.start()
        @pl.when(jnp.logical_not(patient))
        def _():
            pl.semaphore_wait(barrier, 8)

        pl.semaphore_signal(again, inc=1, device_id=named(other, y, c), device_id_type=MESH)

    early[mine] = sent[0, mine]
    got[mine] = sent[1, mine]

    @pl.when(late)
    def _():
        pl.semaphore_wait(again, 1)

    near = [
        *staying(0, sent.at[0], early),
        *staying(2, tails, heads),
        *staying(1, sent.at[1], got),
    ]
    for copy in near:
        copy.start()

    @pl.when(jnp.logical_not(patient))
    def _():
        turned()

    sorted_taps()

    loads[5].wait()
    loads[6].wait()

    def wait_for(count, near):
        whole(0, early, count, near).wait_recv()
        whole(2, heads, count, near).wait_recv()

    row = lax.rem(lax.broadcasted_iota(jnp.int32, (256, 256), 0), 8)
    column = lax.broadcasted_iota(jnp.int32, (256, 256), 1)
    lane = lax.rem(column, LANES)
    select = jnp.logical_and(lane < 4, row == column // LANES * 4 + lane)
    select = jnp.where(select, 1.0, 0.0).astype(jnp.bfloat16)

    def spread(half):
        some = slice(8 * half, 8 * half + 8)
        picked = [
            jnp.where(chosen, jnp.broadcast_to(heads[s], (16, LANES)), 0.0)
            for s in range(8 * half, 8 * half + 8)
        ]
        added = jnp.dot(
            jnp.concatenate(split(jnp.concatenate(picked, axis=0)), axis=1),
            select,
            preferred_element_type=jnp.float32,
        ).reshape(8, 16, 256)
        over_end[some] = added[:, :, :LANES]
        extra[some] = added[:, :, LANES:]

    def put(half, quarters, add):
        rows = slice(16 * half, 16 * half + 16)
        for d, both in enumerate(quarters):
            lanes = slice(LANES * d, LANES * d + LANES)
            for part, value in enumerate(both):
                value = value.reshape(4, 16, LANES)
                if add:
                    value = value + first[part, :, rows, lanes]
                first[part, :, rows, lanes] = value

    wait_for(7, True)
    whole(1, got, 7, True).wait_recv()

    @pl.when(late)
    def _():
        wait_for(8, False)

    spread(0)
    put(0, classes(0, 0, 16, early, over_end, taps_out, fir, cm, tw), False)

    @pl.when(jnp.logical_not(late))
    def _():
        put(0, classes(1, 0, 16, got, extra, taps_out, fir, cm, tw), True)
        wait_for(8, False)

    spread(1)
    put(1, classes(0, 16, 16, early, over_end, taps_out, fir, cm, tw), False)
    whole(0, early, 15, True).wait_send()
    whole(2, heads, 15, True).wait_send()
    whole(1, got, 8, False).wait_recv()
    whole(1, got, 15, True).wait_send()


def fine_kernel(got, extra, taps, first, cm, tw, out, fir, stage, out_sem):
    late = lax.axis_index("zh") == 1

    def write(source, start, count, k):
        rows = pl.ds(start, count)
        return pltpu.make_async_copy(source.at[:, k, rows], out.at[:, k, rows], out_sem.at[k])

    def finish(start, count):
        rows = slice(start, start + count)
        quarters = classes(1, start, count, got, extra, taps, fir, cm, tw)
        for k in range(4):
            for d, both in enumerate(quarters):
                lanes = slice(LANES * d, LANES * d + LANES)
                for part, value in enumerate(both):
                    stage[part, k, rows, lanes] = (
                        first[part, k, rows, lanes] + value[count * k : count * (k + 1)]
                    )
            write(stage, start, count, k).start()

    @pl.when(jnp.logical_not(late))
    def _():
        for k in range(4):
            write(first, 0, 16, k).start()
        finish(16, 16)

    @pl.when(late)
    def _():
        finish(0, 32)

    for k in range(4):
        write(stage, 0, 32, k).wait()


def on_device(signal, coarse_taps, fine_taps):
    rows = signal.reshape(2, HALF, LANES).transpose(1, 0, 2).reshape(ROWS, LANES)
    hbm = pl.BlockSpec(memory_space=pltpu.HBM)
    vmem = pl.BlockSpec(memory_space=pltpu.VMEM)
    tables = [jnp.asarray(v) for v in (coarse_matrix(), fine_matrix(), twiddles())]
    operands = (rows, tables[0], coarse_taps, fine_taps, *tables[1:])
    f32 = jnp.float32
    handed = pl.pallas_call(
        gather_kernel,
        out_shape=[
            jax.ShapeDtypeStruct((PEERS, 16, 256), f32),
            jax.ShapeDtypeStruct((PEERS, 16, LANES), f32),
            jax.ShapeDtypeStruct((2, FINE_TAPS, 8, LANES), f32),
            jax.ShapeDtypeStruct((2, 4, 32, FINE), f32),
            jax.ShapeDtypeStruct((768, 256), jnp.bfloat16),
            jax.ShapeDtypeStruct((8, LANES), f32),
        ],
        in_specs=[hbm] * 6,
        out_specs=[vmem] * 6,
        scratch_shapes=[
            pltpu.VMEM((HEAD + ROWS + TAIL, LANES), f32),
            pltpu.VMEM((HEAD + ROWS + TAIL, LANES), f32),
            pltpu.VMEM((256, 512), jnp.bfloat16),
            pltpu.VMEM((TAPS, CHANNELS), f32),
            pltpu.VMEM((FINE_TAPS, FINE), f32),
            pltpu.VMEM((FINE, LANES), f32),
            pltpu.VMEM((PEERS, 16, 256), f32),
            pltpu.VMEM((PEERS, 1, LANES), f32),
            pltpu.VMEM((PEERS, 1, LANES), f32),
            pltpu.VMEM((2, PEERS, 16, 256), f32),
            pltpu.VMEM((PEERS, 16, LANES), f32),
            pltpu.VMEM((2, LANES, LANES), f32),
            pltpu.SemaphoreType.DMA((7,)),
            pltpu.SemaphoreType.DMA((3,)),
            pltpu.SemaphoreType.DMA((6,)),
            pltpu.SemaphoreType.REGULAR((8,)),
            pltpu.SemaphoreType.REGULAR,
        ],
        compiler_params=pltpu.CompilerParams(
            collective_id=0, has_side_effects=True, vmem_limit_bytes=16 << 20
        ),
        name="gather",
    )(*(pltpu.with_memory_space_constraint(v, pltpu.HBM) for v in operands))
    return pl.pallas_call(
        fine_kernel,
        out_shape=jax.ShapeDtypeStruct((2, 4, 32, FINE), f32),
        in_specs=[vmem] * 6,
        out_specs=hbm,
        scratch_shapes=[
            pltpu.VMEM((2, 256, LANES), f32),
            pltpu.VMEM((2, 4, 32, FINE), f32),
            pltpu.SemaphoreType.DMA((4,)),
        ],
        compiler_params=pltpu.CompilerParams(vmem_limit_bytes=16 << 20),
        name="fine",
    )(*handed)


def solution(mesh):
    finer = Mesh(mesh.devices.reshape(mesh.shape["streams"], *GROUP), ("streams", *TM))
    return jax.shard_map(
        on_device,
        mesh=finer,
        in_specs=(P(None, ("streams", *TM)), P(), P()),
        out_specs=P(None, TM, "streams", None),
        check_vma=False,
    )
```

```python
import functools
import math

import jax
import jax.numpy as jnp
import numpy as np
from jax import lax
from jax.experimental import pallas as pl
from jax.experimental.pallas import tpu as pltpu
from jax.sharding import Mesh
from jax.sharding import PartitionSpec as P

CHANNELS = 64
FINE = 512
TAPS = 16
FINE_TAPS = 12
TM = ("zh", "y", "c")
GROUP = (2, 4, 2)
PEERS = 16
LANES = 128
HEAD = 16
TAIL = 40
ROWS = 1024
HALF = 512
MESH = pl.DeviceIdType.MESH
BESIDE = [(dy, dc) for dy in (2, 1, 3, 0) for dc in (1, 0) if (dy, dc) != (0, 0)]


def split(value):
    high = value.astype(jnp.bfloat16)
    low = (value - high.astype(jnp.float32)).astype(jnp.bfloat16)
    return high, low


def np_split(value):
    value = value.astype(np.float32)
    high = value.astype(jnp.bfloat16)
    low = (value - high.astype(np.float32)).astype(jnp.bfloat16)
    return high, low


def coarse_matrix():
    owner, part, own, parity = np.meshgrid(
        np.arange(16), np.arange(2), np.arange(4), np.arange(2), indexing="ij"
    )
    channel = (4 * owner + own).reshape(-1, 1)
    part, parity = part.reshape(-1, 1), parity.reshape(-1, 1)
    part_in, parity_in, branch = np.meshgrid(
        np.arange(2), np.arange(2), np.arange(CHANNELS), indexing="ij"
    )
    part_in, parity_in, branch = (v.reshape(1, -1) for v in (part_in, parity_in, branch))
    angle = 2.0 * np.pi * (channel * branch % CHANNELS) / CHANNELS
    value = np.where(part == part_in, np.cos(angle), np.sin(angle) * (part_in - part))
    value = np.where(parity == parity_in, value, 0.0) / math.sqrt(CHANNELS)
    return np.concatenate(np_split(value), axis=1)


def fine_matrix():
    part_in, b = np.meshgrid(np.arange(2), np.arange(LANES), indexing="ij")
    part_in, b = part_in.reshape(-1, 1), b.reshape(-1, 1)
    part, c = part_in.reshape(1, -1), b.reshape(1, -1)
    angle = 2.0 * np.pi * (b * c % LANES) / LANES
    value = np.where(part == part_in, np.cos(angle), np.sin(angle) * (part_in - part))
    high, low = np_split(value / math.sqrt(FINE))
    return np.concatenate([high, low, high], axis=0)


def twiddles():
    a, c = np.meshgrid(np.arange(4), np.arange(LANES), indexing="ij")
    angle = 2.0 * np.pi * a * c / FINE
    return np.concatenate([np.cos(angle), np.sin(angle)]).astype(np.float32)


def flat(zh, y, c):
    return (zh * 4 + y) * 2 + c


def named(zh, y, c):
    return {"zh": zh, "y": y, "c": c}


def coarse_frames(xs, ys, taps, start, size):
    parts = []
    for c in range(2):
        acc = None
        for i in range(TAPS // 2):
            rows = pl.ds(HEAD + start + c - 2 * i, size, stride=4)
            term = taps[2 * i : 2 * i + 1] * xs[rows, :]
            acc = term if acc is None else acc + term
            acc = acc + taps[2 * i + 1 : 2 * i + 2] * ys[rows, :]
        parts.append(acc)
    return jnp.concatenate(parts, axis=1)


def spectra(ms, frames):
    high, low = split(frames)
    dims = (((1,), (1,)), ((), ()))
    right = jnp.concatenate([high, high], axis=1)
    result = lax.dot_general(ms[...], right, dims, preferred_element_type=jnp.float32)
    return result + lax.dot_general(
        ms[:, 0:256], low, dims, preferred_element_type=jnp.float32
    )


def fine_filter(start, count, block, taps, fir):
    for c in range(2):
        blocks = {}
        for frame in range(start, start + count):
            acc = None
            for j in range(min(FINE_TAPS, frame + 1)):
                at = frame - j
                if at not in blocks:
                    blocks[at] = block(c, at)
                term = taps(j) * blocks[at]
                acc = term if acc is None else acc + term
            fir[c, pl.ds(8 * (frame - start), 8), :] = acc


def fine_spectra(a1, count, fir, cm, tw):
    rows = []
    for h in range(2):
        for k in range(4):
            parts = [fir[c, pl.ds(2 * k + h, count, stride=8), :] for c in range(2)]
            rows.append(jnp.concatenate(parts, axis=1))
    high, low = split(jnp.concatenate(rows, axis=0))
    left = jnp.concatenate([high, high, low], axis=1)
    spectrum = jnp.dot(left, cm[...], preferred_element_type=jnp.float32)
    result = []
    for h in range(2):
        a = 2 * a1 + h
        rows = slice(4 * count * h, 4 * count * (h + 1))
        re, im = spectrum[rows, :LANES], spectrum[rows, LANES:]
        if a:
            cos, sin = tw[a : a + 1, :], tw[4 + a : 5 + a, :]
            re, im = re * cos + im * sin, im * cos - re * sin
        result.append((re, im))
    (re0, im0), (re1, im1) = result
    quarters = [
        (re0 + re1, im0 + im1),
        (re0 + im1, im0 - re1),
        (re0 - re1, im0 - im1),
        (re0 - im1, im0 + re1),
    ]
    if a1:
        quarters = [(-re, -im) if d % 2 else (re, im) for d, (re, im) in enumerate(quarters)]
    return quarters


def classes(a1, start, count, blocks, over_end, taps, fir, cm, tw):
    def block(c, frame):
        value = blocks[frame // 2, pl.ds(8 * c, 8), pl.ds(LANES * (frame % 2), LANES)]
        if frame % 2 == 0 and frame > 0:
            value = value + over_end[frame // 2 - 1, pl.ds(8 * c, 8), :]
        return value

    fine_filter(start, count, block, lambda j: taps[a1, j], fir)
    return fine_spectra(a1, count, fir, cm, tw)


def gather_kernel(
    x_hbm, m_hbm, ct_hbm, ft_hbm, c_hbm, t_hbm, got, extra, taps_out, first, cm, tw,
    xs, ys, ms, ct, ft, ftt, early, tails, heads, sent, over_end, fir,
    load_sem, send_sem, recv_sem, ready, again,
):
    loads = [
        pltpu.make_async_copy(ct_hbm, ct, load_sem.at[0]),
        pltpu.make_async_copy(
            x_hbm.at[pl.ds(0, HALF)], xs.at[pl.ds(HEAD, HALF)], load_sem.at[1]
        ),
        pltpu.make_async_copy(
            x_hbm.at[pl.ds(HALF, HALF)], xs.at[pl.ds(HEAD + HALF, HALF)], load_sem.at[2]
        ),
        pltpu.make_async_copy(m_hbm, ms, load_sem.at[3]),
        pltpu.make_async_copy(ft_hbm, ft, load_sem.at[4]),
        pltpu.make_async_copy(c_hbm, cm, load_sem.at[5]),
        pltpu.make_async_copy(t_hbm, tw, load_sem.at[6]),
    ]
    for load in loads[:4]:
        load.start()
    zh, y, c = (lax.axis_index(axis) for axis in TM)
    mine = flat(zh, y, c)
    own = 2 * y + c
    other = 1 - zh
    late = zh == 1
    patient = jnp.logical_and(zh == 0, lax.div(lax.axis_index("streams"), 4) == 1)
    turn = lax.rem(lax.div(y + 1, 2), 2)
    def pick(*table):
        by_y = [jnp.where(y == 2, t[2], t[3]) for t in zip(*table, strict=True)]
        by_y = [jnp.where(y == 1, t[1], v) for t, v in zip(zip(*table), by_y, strict=True)]
        return [jnp.where(y == 0, t[0], v) for t, v in zip(zip(*table), by_y, strict=True)]

    to_early = pick((2, 1, 0, 3), (3, 0, 1, 2), (0, 1, 3, 2), (1, 0, 2, 3))
    to_late = [turn, 1 - turn, 2 + turn, 3 - turn]
    order = [jnp.where(late, p, q) for p, q in zip(to_early, to_late, strict=True)]
    across = [(dy, dc) for dy in order for dc in (1, 0)]
    barrier = pltpu.get_barrier_semaphore()
    for at in across:
        pl.semaphore_signal(barrier, inc=1, device_id=named(other, *at), device_id_type=MESH)

    @pl.when(late)
    def _():
        pl.semaphore_wait(barrier, 8)
        for at in across:
            pl.semaphore_signal(
                ready.at[own], inc=1, device_id=named(other, *at), device_id_type=MESH
            )

    xs[pl.ds(0, HEAD), :] = jnp.zeros((HEAD, LANES), jnp.float32)
    xs[pl.ds(HEAD + ROWS, TAIL), :] = jnp.zeros((TAIL, LANES), jnp.float32)
    ys[pl.ds(0, HEAD), :] = jnp.zeros((HEAD, LANES), jnp.float32)
    loads[0].wait()
    taps = ct[...]
    taps = jnp.concatenate([taps, taps], axis=1)

    def delay(start, size):
        left = lax.broadcasted_iota(jnp.int32, (size, LANES), 1) < CHANNELS
        here = xs[pl.ds(start, size), :]
        before = xs[pl.ds(start - 2, size), :]
        ys[pl.ds(start, size), :] = pltpu.roll(jnp.where(left, here, before), CHANNELS, 1)

    def compute(a1, m):
        frames = coarse_frames(xs, ys, taps, HALF * m + 2 * a1, LANES)
        sent[a1, :, :, LANES * m : LANES * (m + 1)] = spectra(ms, frames).reshape(
            PEERS, 16, LANES
        )

    def turned():
        loads[4].wait()
        square = jnp.concatenate(
            [ft[...], jnp.zeros((LANES - FINE_TAPS, FINE), jnp.float32)], axis=0
        )
        for k in range(4):
            ftt[pl.ds(LANES * k, LANES), :] = square[:, LANES * k : LANES * (k + 1)].T

    def sorted_taps():
        by_branch = [ftt[pl.ds(a, LANES, stride=4), :].T for a in range(4)]
        odd = lax.rem(lax.broadcasted_iota(jnp.int32, (8, LANES), 0), 2) == 1
        for a1 in range(2):
            for j in range(FINE_TAPS):
                even_row = jnp.broadcast_to(by_branch[2 * a1][j : j + 1], (8, LANES))
                odd_row = jnp.broadcast_to(by_branch[2 * a1 + 1][j : j + 1], (8, LANES))
                taps_out[a1, j] = jnp.where(odd, odd_row, even_row)

    def crossing(piece, source, target):
        return [
            pltpu.make_async_remote_copy(
                src_ref=source.at[flat(other, *at)],
                dst_ref=target.at[mine],
                send_sem=send_sem.at[piece],
                recv_sem=recv_sem.at[piece],
                device_id=named(other, *at),
                device_id_type=MESH,
            )
            for at in across
        ]

    def staying(piece, source, target):
        copies = []
        for dy, dc in BESIDE:
            to = (zh, lax.rem(y + dy, 4), lax.rem(c + dc, 2))
            copy = pltpu.make_async_remote_copy(
                src_ref=source.at[flat(*to)],
                dst_ref=target.at[mine],
                send_sem=send_sem.at[piece],
                recv_sem=recv_sem.at[piece + 3],
                device_id=named(*to),
                device_id_type=MESH,
            )
            copies.append(copy)
        return copies

    def whole(piece, target, count, near):
        return pltpu.make_async_remote_copy(
            src_ref=target.at[pl.ds(0, count)],
            dst_ref=target.at[pl.ds(0, count)],
            send_sem=send_sem.at[piece],
            recv_sem=recv_sem.at[piece + 3 * near],
            device_id=named(other, y, c),
            device_id_type=MESH,
        )

    def part(m, at):
        return pltpu.make_async_remote_copy(
            src_ref=sent.at[0, flat(other, *at), :, pl.ds(LANES * m, LANES)],
            dst_ref=early.at[mine, :, pl.ds(LANES * m, LANES)],
            send_sem=send_sem.at[0],
            recv_sem=recv_sem.at[0],
            device_id=named(other, *at),
            device_id_type=MESH,
        )

    zero = crossing(0, sent.at[0], early)
    one = crossing(1, sent.at[1], got)
    two = crossing(2, tails, heads)

    def start(copies):
        @pl.when(late)
        def _():
            for copy in copies:
                copy.start()

    loads[1].wait()
    delay(HEAD, HALF)
    loads[3].wait()
    compute(0, 0)
    start([part(0, at) for at in across[:4]])
    loads[2].wait()
    delay(HEAD + HALF, HALF + TAIL)
    compute(0, 1)
    start([part(1, at) for at in across[:4]])
    for load in loads[4:]:
        load.start()
    compute(1, 0)
    compute(1, 1)
    start(one[:4])

    ends = [coarse_frames(xs, ys, taps, ROWS + 2 * a1, 8) for a1 in range(2)]
    lower = lax.broadcasted_iota(jnp.int32, (8, 256), 0) < 4
    ends = jnp.where(lower, ends[0], pltpu.roll(ends[1], 4, 0))
    result = spectra(ms, jnp.concatenate([ends] * 16, axis=0))
    chosen = (
        lax.broadcasted_iota(jnp.int32, (16, LANES), 1) // 8
        == lax.broadcasted_iota(jnp.int32, (16, LANES), 0)
    )
    for d in range(PEERS):
        picked = jnp.where(chosen, result[16 * d : 16 * d + 16], 0.0)
        tails[d] = jnp.sum(picked, axis=0, keepdims=True)
    heads[mine] = tails[mine]
    start([*two, *zero[4:], *one[4:]])

    @pl.when(jnp.logical_not(late))
    def _():
        @pl.when(patient)
        def _():
            pl.semaphore_wait(barrier, 8)
            turned()

        for half in (slice(0, 4), slice(4, 8)):
            for at, copy in zip(across[half], zero[half], strict=True):
                pl.semaphore_wait(ready.at[flat(0, *at)], 1)
                copy.start()
            for copy in (*two[half], *one[half]):
                copy.start()
        @pl.when(jnp.logical_not(patient))
        def _():
            pl.semaphore_wait(barrier, 8)

        pl.semaphore_signal(again, inc=1, device_id=named(other, y, c), device_id_type=MESH)

    early[mine] = sent[0, mine]
    got[mine] = sent[1, mine]

    @pl.when(late)
    def _():
        pl.semaphore_wait(again, 1)

    near = [
        *staying(0, sent.at[0], early),
        *staying(2, tails, heads),
        *staying(1, sent.at[1], got),
    ]
    for copy in near:
        copy.start()

    @pl.when(jnp.logical_not(patient))
    def _():
        turned()

    sorted_taps()

    loads[5].wait()
    loads[6].wait()

    row = lax.rem(lax.broadcasted_iota(jnp.int32, (256, 256), 0), 8)
    column = lax.broadcasted_iota(jnp.int32, (256, 256), 1)
    lane = lax.rem(column, LANES)
    select = jnp.logical_and(lane < 4, row == column // LANES * 4 + lane)
    select = jnp.where(select, 1.0, 0.0).astype(jnp.bfloat16)

    def spread(half):
        some = slice(8 * half, 8 * half + 8)
        picked = [
            jnp.where(chosen, jnp.broadcast_to(heads[s], (16, LANES)), 0.0)
            for s in range(8 * half, 8 * half + 8)
        ]
        added = jnp.dot(
            jnp.concatenate(split(jnp.concatenate(picked, axis=0)), axis=1),
            select,
            preferred_element_type=jnp.float32,
        ).reshape(8, 16, 256)
        over_end[some] = added[:, :, :LANES]
        extra[some] = added[:, :, LANES:]

    def put(half, quarters, add):
        rows = slice(16 * half, 16 * half + 16)
        for d, both in enumerate(quarters):
            lanes = slice(LANES * d, LANES * d + LANES)
            for part, value in enumerate(both):
                value = value.reshape(4, 16, LANES)
                if add:
                    value = value + first[part, :, rows, lanes]
                first[part, :, rows, lanes] = value

    whole(0, early, 7, True).wait_recv()
    whole(1, got, 7, True).wait_recv()
    whole(2, heads, 7, True).wait_recv()

    @pl.when(late)
    def _():
        whole(2, heads, 8, False).wait_recv()
        spread(1)
        whole(0, early, 8, False).wait_recv()

    spread(0)
    put(0, classes(0, 0, 16, early, over_end, taps_out, fir, cm, tw), False)

    @pl.when(jnp.logical_not(late))
    def _():
        put(0, classes(1, 0, 16, got, extra, taps_out, fir, cm, tw), True)
        whole(2, heads, 8, False).wait_recv()
        spread(1)
        whole(0, early, 8, False).wait_recv()

    put(1, classes(0, 16, 16, early, over_end, taps_out, fir, cm, tw), False)
    whole(0, early, 15, True).wait_send()
    whole(2, heads, 15, True).wait_send()
    whole(1, got, 8, False).wait_recv()
    whole(1, got, 15, True).wait_send()


def fine_kernel(got, extra, taps, first, cm, tw, out, fir, stage, out_sem):
    late = lax.axis_index("zh") == 1

    def write(source, start, count, k):
        rows = pl.ds(start, count)
        return pltpu.make_async_copy(source.at[:, k, rows], out.at[:, k, rows], out_sem.at[k])

    def finish(start, count):
        rows = slice(start, start + count)
        quarters = classes(1, start, count, got, extra, taps, fir, cm, tw)
        for k in range(4):
            for d, both in enumerate(quarters):
                lanes = slice(LANES * d, LANES * d + LANES)
                for part, value in enumerate(both):
                    stage[part, k, rows, lanes] = (
                        first[part, k, rows, lanes] + value[count * k : count * (k + 1)]
                    )
            write(stage, start, count, k).start()

    @pl.when(jnp.logical_not(late))
    def _():
        for k in range(4):
            write(first, 0, 16, k).start()
        finish(16, 16)

    @pl.when(late)
    def _():
        finish(0, 32)

    for k in range(4):
        write(stage, 0, 32, k).wait()


def on_device(signal, coarse_taps, fine_taps):
    rows = signal.reshape(2, HALF, LANES).transpose(1, 0, 2).reshape(ROWS, LANES)
    hbm = pl.BlockSpec(memory_space=pltpu.HBM)
    vmem = pl.BlockSpec(memory_space=pltpu.VMEM)
    tables = [jnp.asarray(v) for v in (coarse_matrix(), fine_matrix(), twiddles())]
    operands = (rows, tables[0], coarse_taps, fine_taps, *tables[1:])
    f32 = jnp.float32
    handed = pl.pallas_call(
        gather_kernel,
        out_shape=[
            jax.ShapeDtypeStruct((PEERS, 16, 256), f32),
            jax.ShapeDtypeStruct((PEERS, 16, LANES), f32),
            jax.ShapeDtypeStruct((2, FINE_TAPS, 8, LANES), f32),
            jax.ShapeDtypeStruct((2, 4, 32, FINE), f32),
            jax.ShapeDtypeStruct((768, 256), jnp.bfloat16),
            jax.ShapeDtypeStruct((8, LANES), f32),
        ],
        in_specs=[hbm] * 6,
        out_specs=[vmem] * 6,
        scratch_shapes=[
            pltpu.VMEM((HEAD + ROWS + TAIL, LANES), f32),
            pltpu.VMEM((HEAD + ROWS + TAIL, LANES), f32),
            pltpu.VMEM((256, 512), jnp.bfloat16),
            pltpu.VMEM((TAPS, CHANNELS), f32),
            pltpu.VMEM((FINE_TAPS, FINE), f32),
            pltpu.VMEM((FINE, LANES), f32),
            pltpu.VMEM((PEERS, 16, 256), f32),
            pltpu.VMEM((PEERS, 1, LANES), f32),
            pltpu.VMEM((PEERS, 1, LANES), f32),
            pltpu.VMEM((2, PEERS, 16, 256), f32),
            pltpu.VMEM((PEERS, 16, LANES), f32),
            pltpu.VMEM((2, LANES, LANES), f32),
            pltpu.SemaphoreType.DMA((7,)),
            pltpu.SemaphoreType.DMA((3,)),
            pltpu.SemaphoreType.DMA((6,)),
            pltpu.SemaphoreType.REGULAR((8,)),
            pltpu.SemaphoreType.REGULAR,
        ],
        compiler_params=pltpu.CompilerParams(
            collective_id=0, has_side_effects=True, vmem_limit_bytes=16 << 20
        ),
        name="gather",
    )(*(pltpu.with_memory_space_constraint(v, pltpu.HBM) for v in operands))
    return pl.pallas_call(
        fine_kernel,
        out_shape=jax.ShapeDtypeStruct((2, 4, 32, FINE), f32),
        in_specs=[vmem] * 6,
        out_specs=hbm,
        scratch_shapes=[
            pltpu.VMEM((2, 256, LANES), f32),
            pltpu.VMEM((2, 4, 32, FINE), f32),
            pltpu.SemaphoreType.DMA((4,)),
        ],
        compiler_params=pltpu.CompilerParams(vmem_limit_bytes=16 << 20),
        name="fine",
    )(*handed)


def solution(mesh):
    finer = Mesh(mesh.devices.reshape(mesh.shape["streams"], *GROUP), ("streams", *TM))
    return jax.shard_map(
        on_device,
        mesh=finer,
        in_specs=(P(None, ("streams", *TM)), P(), P()),
        out_specs=P(None, TM, "streams", None),
        check_vma=False,
    )
```

```python
import functools
import math

import jax
import jax.numpy as jnp
import numpy as np
from jax import lax
from jax.experimental import pallas as pl
from jax.experimental.pallas import tpu as pltpu
from jax.sharding import Mesh
from jax.sharding import PartitionSpec as P

CHANNELS = 64
FINE = 512
TAPS = 16
FINE_TAPS = 12
TM = ("zh", "y", "c")
GROUP = (2, 4, 2)
PEERS = 16
LANES = 128
HEAD = 16
TAIL = 40
ROWS = 1024
HALF = 512
MESH = pl.DeviceIdType.MESH
BESIDE = [(dy, dc) for dy in (2, 1, 3, 0) for dc in (1, 0) if (dy, dc) != (0, 0)]


def split(value):
    high = value.astype(jnp.bfloat16)
    low = (value - high.astype(jnp.float32)).astype(jnp.bfloat16)
    return high, low


def np_split(value):
    value = value.astype(np.float32)
    high = value.astype(jnp.bfloat16)
    low = (value - high.astype(np.float32)).astype(jnp.bfloat16)
    return high, low


def coarse_matrix():
    owner, part, own, parity = np.meshgrid(
        np.arange(16), np.arange(2), np.arange(4), np.arange(2), indexing="ij"
    )
    channel = (4 * owner + own).reshape(-1, 1)
    part, parity = part.reshape(-1, 1), parity.reshape(-1, 1)
    part_in, parity_in, branch = np.meshgrid(
        np.arange(2), np.arange(2), np.arange(CHANNELS), indexing="ij"
    )
    part_in, parity_in, branch = (v.reshape(1, -1) for v in (part_in, parity_in, branch))
    angle = 2.0 * np.pi * (channel * branch % CHANNELS) / CHANNELS
    value = np.where(part == part_in, np.cos(angle), np.sin(angle) * (part_in - part))
    value = np.where(parity == parity_in, value, 0.0) / math.sqrt(CHANNELS)
    return np.concatenate(np_split(value), axis=1)


def fine_matrix():
    part_in, b = np.meshgrid(np.arange(2), np.arange(LANES), indexing="ij")
    part_in, b = part_in.reshape(-1, 1), b.reshape(-1, 1)
    part, c = part_in.reshape(1, -1), b.reshape(1, -1)
    angle = 2.0 * np.pi * (b * c % LANES) / LANES
    value = np.where(part == part_in, np.cos(angle), np.sin(angle) * (part_in - part))
    high, low = np_split(value / math.sqrt(FINE))
    return np.concatenate([high, low, high], axis=0)


def twiddles():
    a, c = np.meshgrid(np.arange(4), np.arange(LANES), indexing="ij")
    angle = 2.0 * np.pi * a * c / FINE
    return np.concatenate([np.cos(angle), np.sin(angle)]).astype(np.float32)


def flat(zh, y, c):
    return (zh * 4 + y) * 2 + c


def named(zh, y, c):
    return {"zh": zh, "y": y, "c": c}


def coarse_frames(xs, ys, taps, start, size):
    parts = []
    for c in range(2):
        acc = None
        for i in range(TAPS // 2):
            rows = pl.ds(HEAD + start + c - 2 * i, size, stride=4)
            term = taps[2 * i : 2 * i + 1] * xs[rows, :]
            acc = term if acc is None else acc + term
            acc = acc + taps[2 * i + 1 : 2 * i + 2] * ys[rows, :]
        parts.append(acc)
    return jnp.concatenate(parts, axis=1)


def spectra(ms, frames):
    high, low = split(frames)
    dims = (((1,), (1,)), ((), ()))
    right = jnp.concatenate([high, high], axis=1)
    result = lax.dot_general(ms[...], right, dims, preferred_element_type=jnp.float32)
    return result + lax.dot_general(
        ms[:, 0:256], low, dims, preferred_element_type=jnp.float32
    )


def fine_filter(start, count, block, taps, fir):
    for c in range(2):
        blocks = {}
        for frame in range(start, start + count):
            acc = None
            for j in range(min(FINE_TAPS, frame + 1)):
                at = frame - j
                if at not in blocks:
                    blocks[at] = block(c, at)
                term = taps(j) * blocks[at]
                acc = term if acc is None else acc + term
            fir[c, pl.ds(8 * (frame - start), 8), :] = acc


def fine_spectra(a1, count, fir, cm, tw):
    rows = []
    for h in range(2):
        for k in range(4):
            parts = [fir[c, pl.ds(2 * k + h, count, stride=8), :] for c in range(2)]
            rows.append(jnp.concatenate(parts, axis=1))
    high, low = split(jnp.concatenate(rows, axis=0))
    left = jnp.concatenate([high, high, low], axis=1)
    spectrum = jnp.dot(left, cm[...], preferred_element_type=jnp.float32)
    result = []
    for h in range(2):
        a = 2 * a1 + h
        rows = slice(4 * count * h, 4 * count * (h + 1))
        re, im = spectrum[rows, :LANES], spectrum[rows, LANES:]
        if a:
            cos, sin = tw[a : a + 1, :], tw[4 + a : 5 + a, :]
            re, im = re * cos + im * sin, im * cos - re * sin
        result.append((re, im))
    (re0, im0), (re1, im1) = result
    quarters = [
        (re0 + re1, im0 + im1),
        (re0 + im1, im0 - re1),
        (re0 - re1, im0 - im1),
        (re0 - im1, im0 + re1),
    ]
    if a1:
        quarters = [(-re, -im) if d % 2 else (re, im) for d, (re, im) in enumerate(quarters)]
    return quarters


def classes(a1, start, count, blocks, over_end, taps, fir, cm, tw):
    def block(c, frame):
        value = blocks[frame // 2, pl.ds(8 * c, 8), pl.ds(LANES * (frame % 2), LANES)]
        if frame % 2 == 0 and frame > 0:
            value = value + over_end[frame // 2 - 1, pl.ds(8 * c, 8), :]
        return value

    fine_filter(start, count, block, lambda j: taps[a1, j], fir)
    return fine_spectra(a1, count, fir, cm, tw)


def gather_kernel(
    x_hbm, m_hbm, ct_hbm, ft_hbm, c_hbm, t_hbm, got, extra, taps_out, first, cm, tw,
    xs, ys, ms, ct, ft, ftt, early, tails, heads, sent, over_end, fir,
    load_sem, send_sem, recv_sem, ready, again,
):
    loads = [
        pltpu.make_async_copy(ct_hbm, ct, load_sem.at[0]),
        pltpu.make_async_copy(
            x_hbm.at[pl.ds(0, HALF)], xs.at[pl.ds(HEAD, HALF)], load_sem.at[1]
        ),
        pltpu.make_async_copy(
            x_hbm.at[pl.ds(HALF, HALF)], xs.at[pl.ds(HEAD + HALF, HALF)], load_sem.at[2]
        ),
        pltpu.make_async_copy(m_hbm, ms, load_sem.at[3]),
        pltpu.make_async_copy(ft_hbm, ft, load_sem.at[4]),
        pltpu.make_async_copy(c_hbm, cm, load_sem.at[5]),
        pltpu.make_async_copy(t_hbm, tw, load_sem.at[6]),
    ]
    for k in (1, 0, 3, 2):
        loads[k].start()
    zh, y, c = (lax.axis_index(axis) for axis in TM)
    mine = flat(zh, y, c)
    own = 2 * y + c
    other = 1 - zh
    late = zh == 1
    patient = jnp.logical_and(zh == 0, lax.div(lax.axis_index("streams"), 4) == 1)
    turn = lax.rem(lax.div(y + 1, 2), 2)
    def pick(*table):
        by_y = [jnp.where(y == 2, t[2], t[3]) for t in zip(*table, strict=True)]
        by_y = [jnp.where(y == 1, t[1], v) for t, v in zip(zip(*table), by_y, strict=True)]
        return [jnp.where(y == 0, t[0], v) for t, v in zip(zip(*table), by_y, strict=True)]

    to_early = pick((2, 1, 0, 3), (3, 0, 1, 2), (1, 0, 3, 2), (0, 1, 2, 3))
    to_late = [turn, 1 - turn, 2 + turn, 3 - turn]
    order = [jnp.where(late, p, q) for p, q in zip(to_early, to_late, strict=True)]
    across = [(dy, dc) for dy in order for dc in (1, 0)]
    barrier = pltpu.get_barrier_semaphore()
    for at in across:
        pl.semaphore_signal(barrier, inc=1, device_id=named(other, *at), device_id_type=MESH)

    @pl.when(late)
    def _():
        pl.semaphore_wait(barrier, 8)
        for at in across:
            pl.semaphore_signal(
                ready.at[own], inc=1, device_id=named(other, *at), device_id_type=MESH
            )

    xs[pl.ds(0, HEAD), :] = jnp.zeros((HEAD, LANES), jnp.float32)
    xs[pl.ds(HEAD + ROWS, TAIL), :] = jnp.zeros((TAIL, LANES), jnp.float32)
    ys[pl.ds(0, HEAD), :] = jnp.zeros((HEAD, LANES), jnp.float32)
    loads[0].wait()
    taps = ct[...]
    taps = jnp.concatenate([taps, taps], axis=1)

    def delay(start, size):
        left = lax.broadcasted_iota(jnp.int32, (size, LANES), 1) < CHANNELS
        here = xs[pl.ds(start, size), :]
        before = xs[pl.ds(start - 2, size), :]
        ys[pl.ds(start, size), :] = pltpu.roll(jnp.where(left, here, before), CHANNELS, 1)

    def compute(a1, m):
        frames = coarse_frames(xs, ys, taps, HALF * m + 2 * a1, LANES)
        sent[a1, :, :, LANES * m : LANES * (m + 1)] = spectra(ms, frames).reshape(
            PEERS, 16, LANES
        )

    def turned():
        loads[4].wait()
        square = jnp.concatenate(
            [ft[...], jnp.zeros((LANES - FINE_TAPS, FINE), jnp.float32)], axis=0
        )
        for k in range(4):
            ftt[pl.ds(LANES * k, LANES), :] = square[:, LANES * k : LANES * (k + 1)].T

    def sorted_taps():
        by_branch = [ftt[pl.ds(a, LANES, stride=4), :].T for a in range(4)]
        odd = lax.rem(lax.broadcasted_iota(jnp.int32, (8, LANES), 0), 2) == 1
        for a1 in range(2):
            for j in range(FINE_TAPS):
                even_row = jnp.broadcast_to(by_branch[2 * a1][j : j + 1], (8, LANES))
                odd_row = jnp.broadcast_to(by_branch[2 * a1 + 1][j : j + 1], (8, LANES))
                taps_out[a1, j] = jnp.where(odd, odd_row, even_row)

    def crossing(piece, source, target):
        return [
            pltpu.make_async_remote_copy(
                src_ref=source.at[flat(other, *at)],
                dst_ref=target.at[mine],
                send_sem=send_sem.at[piece],
                recv_sem=recv_sem.at[piece],
                device_id=named(other, *at),
                device_id_type=MESH,
            )
            for at in across
        ]

    def staying(piece, source, target):
        copies = []
        for dy, dc in BESIDE:
            to = (zh, lax.rem(y + dy, 4), lax.rem(c + dc, 2))
            copy = pltpu.make_async_remote_copy(
                src_ref=source.at[flat(*to)],
                dst_ref=target.at[mine],
                send_sem=send_sem.at[piece],
                recv_sem=recv_sem.at[piece + 3],
                device_id=named(*to),
                device_id_type=MESH,
            )
            copies.append(copy)
        return copies

    def whole(piece, target, count, near):
        return pltpu.make_async_remote_copy(
            src_ref=target.at[pl.ds(0, count)],
            dst_ref=target.at[pl.ds(0, count)],
            send_sem=send_sem.at[piece],
            recv_sem=recv_sem.at[piece + 3 * near],
            device_id=named(other, y, c),
            device_id_type=MESH,
        )

    def part(m, at):
        return pltpu.make_async_remote_copy(
            src_ref=sent.at[0, flat(other, *at), :, pl.ds(LANES * m, LANES)],
            dst_ref=early.at[mine, :, pl.ds(LANES * m, LANES)],
            send_sem=send_sem.at[0],
            recv_sem=recv_sem.at[0],
            device_id=named(other, *at),
            device_id_type=MESH,
        )

    zero = crossing(0, sent.at[0], early)
    one = crossing(1, sent.at[1], got)
    two = crossing(2, tails, heads)

    def start(copies):
        @pl.when(late)
        def _():
            for copy in copies:
                copy.start()

    loads[1].wait()
    delay(HEAD, HALF)
    loads[3].wait()
    compute(0, 0)
    start([part(0, at) for at in across[:4]])
    loads[2].wait()
    delay(HEAD + HALF, HALF + TAIL)
    compute(0, 1)
    start([part(1, at) for at in across[:4]])
    for load in loads[4:]:
        load.start()
    compute(1, 0)
    compute(1, 1)
    start(one[:4])

    ends = [coarse_frames(xs, ys, taps, ROWS + 2 * a1, 8) for a1 in range(2)]
    lower = lax.broadcasted_iota(jnp.int32, (8, 256), 0) < 4
    ends = jnp.where(lower, ends[0], pltpu.roll(ends[1], 4, 0))
    result = spectra(ms, jnp.concatenate([ends] * 16, axis=0))
    chosen = (
        lax.broadcasted_iota(jnp.int32, (16, LANES), 1) // 8
        == lax.broadcasted_iota(jnp.int32, (16, LANES), 0)
    )
    for d in range(PEERS):
        picked = jnp.where(chosen, result[16 * d : 16 * d + 16], 0.0)
        tails[d] = jnp.sum(picked, axis=0, keepdims=True)
    heads[mine] = tails[mine]
    start([*two, *zero[4:], *one[4:]])

    @pl.when(jnp.logical_not(late))
    def _():
        @pl.when(patient)
        def _():
            pl.semaphore_wait(barrier, 8)
            turned()

        for half in (slice(0, 4), slice(4, 8)):
            for at, copy in zip(across[half], zero[half], strict=True):
                pl.semaphore_wait(ready.at[flat(0, *at)], 1)
                copy.start()
            for copy in (*two[half], *one[half]):
                copy.start()
        @pl.when(jnp.logical_not(patient))
        def _():
            pl.semaphore_wait(barrier, 8)

        pl.semaphore_signal(again, inc=1, device_id=named(other, y, c), device_id_type=MESH)

    early[mine] = sent[0, mine]
    got[mine] = sent[1, mine]

    @pl.when(late)
    def _():
        pl.semaphore_wait(again, 1)

    near = [
        *staying(0, sent.at[0], early),
        *staying(2, tails, heads),
        *staying(1, sent.at[1], got),
    ]
    for copy in near:
        copy.start()

    @pl.when(jnp.logical_not(patient))
    def _():
        turned()

    sorted_taps()

    loads[5].wait()
    loads[6].wait()

    row = lax.rem(lax.broadcasted_iota(jnp.int32, (256, 256), 0), 8)
    column = lax.broadcasted_iota(jnp.int32, (256, 256), 1)
    lane = lax.rem(column, LANES)
    select = jnp.logical_and(lane < 4, row == column // LANES * 4 + lane)
    select = jnp.where(select, 1.0, 0.0).astype(jnp.bfloat16)

    def spread(half):
        some = slice(8 * half, 8 * half + 8)
        picked = [
            jnp.where(chosen, jnp.broadcast_to(heads[s], (16, LANES)), 0.0)
            for s in range(8 * half, 8 * half + 8)
        ]
        added = jnp.dot(
            jnp.concatenate(split(jnp.concatenate(picked, axis=0)), axis=1),
            select,
            preferred_element_type=jnp.float32,
        ).reshape(8, 16, 256)
        over_end[some] = added[:, :, :LANES]
        extra[some] = added[:, :, LANES:]

    def put(half, quarters, add):
        rows = slice(16 * half, 16 * half + 16)
        for d, both in enumerate(quarters):
            lanes = slice(LANES * d, LANES * d + LANES)
            for part, value in enumerate(both):
                value = value.reshape(4, 16, LANES)
                if add:
                    value = value + first[part, :, rows, lanes]
                first[part, :, rows, lanes] = value

    whole(0, early, 7, True).wait_recv()
    whole(1, got, 7, True).wait_recv()
    whole(2, heads, 7, True).wait_recv()

    @pl.when(late)
    def _():
        whole(2, heads, 8, False).wait_recv()
        spread(1)
        whole(0, early, 8, False).wait_recv()

    spread(0)
    put(0, classes(0, 0, 16, early, over_end, taps_out, fir, cm, tw), False)

    @pl.when(jnp.logical_not(late))
    def _():
        put(0, classes(1, 0, 16, got, extra, taps_out, fir, cm, tw), True)
        whole(2, heads, 8, False).wait_recv()
        spread(1)
        whole(0, early, 8, False).wait_recv()

    put(1, classes(0, 16, 16, early, over_end, taps_out, fir, cm, tw), False)
    whole(0, early, 15, True).wait_send()
    whole(2, heads, 15, True).wait_send()
    whole(1, got, 8, False).wait_recv()
    whole(1, got, 15, True).wait_send()


def fine_kernel(got, extra, taps, first, cm, tw, out, fir, stage, out_sem):
    late = lax.axis_index("zh") == 1

    def write(source, start, count, k):
        rows = pl.ds(start, count)
        return pltpu.make_async_copy(source.at[:, k, rows], out.at[:, k, rows], out_sem.at[k])

    def finish(start, count):
        rows = slice(start, start + count)
        quarters = classes(1, start, count, got, extra, taps, fir, cm, tw)
        for k in range(4):
            for d, both in enumerate(quarters):
                lanes = slice(LANES * d, LANES * d + LANES)
                for part, value in enumerate(both):
                    stage[part, k, rows, lanes] = (
                        first[part, k, rows, lanes] + value[count * k : count * (k + 1)]
                    )
            write(stage, start, count, k).start()

    @pl.when(jnp.logical_not(late))
    def _():
        for k in range(4):
            write(first, 0, 16, k).start()
        finish(16, 16)

    @pl.when(late)
    def _():
        finish(0, 32)

    for k in range(4):
        write(stage, 0, 32, k).wait()


def on_device(signal, coarse_taps, fine_taps):
    rows = signal.reshape(2, HALF, LANES).transpose(1, 0, 2).reshape(ROWS, LANES)
    hbm = pl.BlockSpec(memory_space=pltpu.HBM)
    vmem = pl.BlockSpec(memory_space=pltpu.VMEM)
    tables = [jnp.asarray(v) for v in (coarse_matrix(), fine_matrix(), twiddles())]
    operands = (rows, tables[0], coarse_taps, fine_taps, *tables[1:])
    f32 = jnp.float32
    handed = pl.pallas_call(
        gather_kernel,
        out_shape=[
            jax.ShapeDtypeStruct((PEERS, 16, 256), f32),
            jax.ShapeDtypeStruct((PEERS, 16, LANES), f32),
            jax.ShapeDtypeStruct((2, FINE_TAPS, 8, LANES), f32),
            jax.ShapeDtypeStruct((2, 4, 32, FINE), f32),
            jax.ShapeDtypeStruct((768, 256), jnp.bfloat16),
            jax.ShapeDtypeStruct((8, LANES), f32),
        ],
        in_specs=[hbm] * 6,
        out_specs=[vmem] * 6,
        scratch_shapes=[
            pltpu.VMEM((HEAD + ROWS + TAIL, LANES), f32),
            pltpu.VMEM((HEAD + ROWS + TAIL, LANES), f32),
            pltpu.VMEM((256, 512), jnp.bfloat16),
            pltpu.VMEM((TAPS, CHANNELS), f32),
            pltpu.VMEM((FINE_TAPS, FINE), f32),
            pltpu.VMEM((FINE, LANES), f32),
            pltpu.VMEM((PEERS, 16, 256), f32),
            pltpu.VMEM((PEERS, 1, LANES), f32),
            pltpu.VMEM((PEERS, 1, LANES), f32),
            pltpu.VMEM((2, PEERS, 16, 256), f32),
            pltpu.VMEM((PEERS, 16, LANES), f32),
            pltpu.VMEM((2, LANES, LANES), f32),
            pltpu.SemaphoreType.DMA((7,)),
            pltpu.SemaphoreType.DMA((3,)),
            pltpu.SemaphoreType.DMA((6,)),
            pltpu.SemaphoreType.REGULAR((8,)),
            pltpu.SemaphoreType.REGULAR,
        ],
        compiler_params=pltpu.CompilerParams(
            collective_id=0, has_side_effects=True, vmem_limit_bytes=16 << 20
        ),
        name="gather",
    )(*(pltpu.with_memory_space_constraint(v, pltpu.HBM) for v in operands))
    return pl.pallas_call(
        fine_kernel,
        out_shape=jax.ShapeDtypeStruct((2, 4, 32, FINE), f32),
        in_specs=[vmem] * 6,
        out_specs=hbm,
        scratch_shapes=[
            pltpu.VMEM((2, 256, LANES), f32),
            pltpu.VMEM((2, 4, 32, FINE), f32),
            pltpu.SemaphoreType.DMA((4,)),
        ],
        compiler_params=pltpu.CompilerParams(vmem_limit_bytes=16 << 20),
        name="fine",
    )(*handed)


def solution(mesh):
    finer = Mesh(mesh.devices.reshape(mesh.shape["streams"], *GROUP), ("streams", *TM))
    return jax.shard_map(
        on_device,
        mesh=finer,
        in_specs=(P(None, ("streams", *TM)), P(), P()),
        out_specs=P(None, TM, "streams", None),
        check_vma=False,
    )
```

```python
import functools
import math

import jax
import jax.numpy as jnp
import numpy as np
from jax import lax
from jax.experimental import pallas as pl
from jax.experimental.pallas import tpu as pltpu
from jax.sharding import Mesh
from jax.sharding import PartitionSpec as P

CHANNELS = 64
FINE = 512
TAPS = 16
FINE_TAPS = 12
TM = ("zh", "y", "c")
GROUP = (2, 4, 2)
PEERS = 16
LANES = 128
HEAD = 16
TAIL = 40
ROWS = 1024
HALF = 512
MESH = pl.DeviceIdType.MESH
BESIDE = [(dy, dc) for dy in (2, 1, 3, 0) for dc in (1, 0) if (dy, dc) != (0, 0)]


def split(value):
    high = value.astype(jnp.bfloat16)
    low = (value - high.astype(jnp.float32)).astype(jnp.bfloat16)
    return high, low


def np_split(value):
    value = value.astype(np.float32)
    high = value.astype(jnp.bfloat16)
    low = (value - high.astype(np.float32)).astype(jnp.bfloat16)
    return high, low


def coarse_matrix():
    owner, part, own, parity = np.meshgrid(
        np.arange(16), np.arange(2), np.arange(4), np.arange(2), indexing="ij"
    )
    channel = (4 * owner + own).reshape(-1, 1)
    part, parity = part.reshape(-1, 1), parity.reshape(-1, 1)
    part_in, parity_in, branch = np.meshgrid(
        np.arange(2), np.arange(2), np.arange(CHANNELS), indexing="ij"
    )
    part_in, parity_in, branch = (v.reshape(1, -1) for v in (part_in, parity_in, branch))
    angle = 2.0 * np.pi * (channel * branch % CHANNELS) / CHANNELS
    value = np.where(part == part_in, np.cos(angle), np.sin(angle) * (part_in - part))
    value = np.where(parity == parity_in, value, 0.0) / math.sqrt(CHANNELS)
    return np.concatenate(np_split(value), axis=1)


def fine_matrix():
    part_in, b = np.meshgrid(np.arange(2), np.arange(LANES), indexing="ij")
    part_in, b = part_in.reshape(-1, 1), b.reshape(-1, 1)
    part, c = part_in.reshape(1, -1), b.reshape(1, -1)
    angle = 2.0 * np.pi * (b * c % LANES) / LANES
    value = np.where(part == part_in, np.cos(angle), np.sin(angle) * (part_in - part))
    high, low = np_split(value / math.sqrt(FINE))
    return np.concatenate([high, low, high], axis=0)


def twiddles():
    a, c = np.meshgrid(np.arange(4), np.arange(LANES), indexing="ij")
    angle = 2.0 * np.pi * a * c / FINE
    return np.concatenate([np.cos(angle), np.sin(angle)]).astype(np.float32)


def flat(zh, y, c):
    return (zh * 4 + y) * 2 + c


def named(zh, y, c):
    return {"zh": zh, "y": y, "c": c}


def coarse_frames(xs, ys, taps, start, size):
    parts = []
    for c in range(2):
        acc = None
        for i in range(TAPS // 2):
            rows = pl.ds(HEAD + start + c - 2 * i, size, stride=4)
            term = taps[2 * i : 2 * i + 1] * xs[rows, :]
            acc = term if acc is None else acc + term
            acc = acc + taps[2 * i + 1 : 2 * i + 2] * ys[rows, :]
        parts.append(acc)
    return jnp.concatenate(parts, axis=1)


def spectra(ms, frames):
    high, low = split(frames)
    dims = (((1,), (1,)), ((), ()))
    right = jnp.concatenate([high, high], axis=1)
    result = lax.dot_general(ms[...], right, dims, preferred_element_type=jnp.float32)
    return result + lax.dot_general(
        ms[:, 0:256], low, dims, preferred_element_type=jnp.float32
    )


def fine_filter(start, count, block, taps, fir):
    for c in range(2):
        blocks = {}
        for frame in range(start, start + count):
            acc = None
            for j in range(min(FINE_TAPS, frame + 1)):
                at = frame - j
                if at not in blocks:
                    blocks[at] = block(c, at)
                term = taps(j) * blocks[at]
                acc = term if acc is None else acc + term
            fir[c, pl.ds(8 * (frame - start), 8), :] = acc


def fine_spectra(a1, count, fir, cm, tw):
    rows = []
    for h in range(2):
        for k in range(4):
            parts = [fir[c, pl.ds(2 * k + h, count, stride=8), :] for c in range(2)]
            rows.append(jnp.concatenate(parts, axis=1))
    high, low = split(jnp.concatenate(rows, axis=0))
    left = jnp.concatenate([high, high, low], axis=1)
    spectrum = jnp.dot(left, cm[...], preferred_element_type=jnp.float32)
    result = []
    for h in range(2):
        a = 2 * a1 + h
        rows = slice(4 * count * h, 4 * count * (h + 1))
        re, im = spectrum[rows, :LANES], spectrum[rows, LANES:]
        if a:
            cos, sin = tw[a : a + 1, :], tw[4 + a : 5 + a, :]
            re, im = re * cos + im * sin, im * cos - re * sin
        result.append((re, im))
    (re0, im0), (re1, im1) = result
    quarters = [
        (re0 + re1, im0 + im1),
        (re0 + im1, im0 - re1),
        (re0 - re1, im0 - im1),
        (re0 - im1, im0 + re1),
    ]
    if a1:
        quarters = [(-re, -im) if d % 2 else (re, im) for d, (re, im) in enumerate(quarters)]
    return quarters


def classes(a1, start, count, blocks, over_end, taps, fir, cm, tw):
    def block(c, frame):
        value = blocks[frame // 2, pl.ds(8 * c, 8), pl.ds(LANES * (frame % 2), LANES)]
        if frame % 2 == 0 and frame > 0:
            value = value + over_end[frame // 2 - 1, pl.ds(8 * c, 8), :]
        return value

    fine_filter(start, count, block, lambda j: taps[a1, j], fir)
    return fine_spectra(a1, count, fir, cm, tw)


def gather_kernel(
    x_hbm, m_hbm, ct_hbm, ft_hbm, c_hbm, t_hbm, got, extra, taps_out, first, cm, tw,
    xs, ys, ms, ct, ft, ftt, early, tails, heads, sent, over_end, fir,
    load_sem, send_sem, recv_sem, ready, again,
):
    loads = [
        pltpu.make_async_copy(ct_hbm, ct, load_sem.at[0]),
        pltpu.make_async_copy(
            x_hbm.at[pl.ds(0, HALF)], xs.at[pl.ds(HEAD, HALF)], load_sem.at[1]
        ),
        pltpu.make_async_copy(
            x_hbm.at[pl.ds(HALF, HALF)], xs.at[pl.ds(HEAD + HALF, HALF)], load_sem.at[2]
        ),
        pltpu.make_async_copy(m_hbm, ms, load_sem.at[3]),
        pltpu.make_async_copy(ft_hbm, ft, load_sem.at[4]),
        pltpu.make_async_copy(c_hbm, cm, load_sem.at[5]),
        pltpu.make_async_copy(t_hbm, tw, load_sem.at[6]),
    ]
    for load in loads[:4]:
        load.start()
    zh, y, c = (lax.axis_index(axis) for axis in TM)
    mine = flat(zh, y, c)
    own = 2 * y + c
    other = 1 - zh
    late = zh == 1
    patient = jnp.logical_and(zh == 0, lax.div(lax.axis_index("streams"), 4) == 1)
    turn = lax.rem(lax.div(y + 1, 2), 2)
    def pick(*table):
        by_y = [jnp.where(y == 2, t[2], t[3]) for t in zip(*table, strict=True)]
        by_y = [jnp.where(y == 1, t[1], v) for t, v in zip(zip(*table), by_y, strict=True)]
        return [jnp.where(y == 0, t[0], v) for t, v in zip(zip(*table), by_y, strict=True)]

    to_early = pick((2, 1, 0, 3), (3, 0, 1, 2), (0, 1, 3, 2), (1, 0, 2, 3))
    to_late = [turn, 1 - turn, 2 + turn, 3 - turn]
    order = [jnp.where(late, p, q) for p, q in zip(to_early, to_late, strict=True)]
    across = [(dy, dc) for dy in order for dc in (1, 0)]
    barrier = pltpu.get_barrier_semaphore()
    for at in across:
        pl.semaphore_signal(barrier, inc=1, device_id=named(other, *at), device_id_type=MESH)

    @pl.when(late)
    def _():
        pl.semaphore_wait(barrier, 8)
        for at in across:
            pl.semaphore_signal(
                ready.at[own], inc=1, device_id=named(other, *at), device_id_type=MESH
            )

    xs[pl.ds(0, HEAD), :] = jnp.zeros((HEAD, LANES), jnp.float32)
    xs[pl.ds(HEAD + ROWS, TAIL), :] = jnp.zeros((TAIL, LANES), jnp.float32)
    ys[pl.ds(0, HEAD), :] = jnp.zeros((HEAD, LANES), jnp.float32)
    loads[0].wait()
    taps = ct[...]
    taps = jnp.concatenate([taps, taps], axis=1)

    def delay(start, size):
        left = lax.broadcasted_iota(jnp.int32, (size, LANES), 1) < CHANNELS
        here = xs[pl.ds(start, size), :]
        before = xs[pl.ds(start - 2, size), :]
        ys[pl.ds(start, size), :] = pltpu.roll(jnp.where(left, here, before), CHANNELS, 1)

    def compute(a1, m):
        frames = coarse_frames(xs, ys, taps, HALF * m + 2 * a1, LANES)
        sent[a1, :, :, LANES * m : LANES * (m + 1)] = spectra(ms, frames).reshape(
            PEERS, 16, LANES
        )

    def turned():
        loads[4].wait()
        square = jnp.concatenate(
            [ft[...], jnp.zeros((LANES - FINE_TAPS, FINE), jnp.float32)], axis=0
        )
        for k in range(4):
            ftt[pl.ds(LANES * k, LANES), :] = square[:, LANES * k : LANES * (k + 1)].T

    def sorted_taps():
        by_branch = [ftt[pl.ds(a, LANES, stride=4), :].T for a in range(4)]
        odd = lax.rem(lax.broadcasted_iota(jnp.int32, (8, LANES), 0), 2) == 1
        for a1 in range(2):
            for j in range(FINE_TAPS):
                even_row = jnp.broadcast_to(by_branch[2 * a1][j : j + 1], (8, LANES))
                odd_row = jnp.broadcast_to(by_branch[2 * a1 + 1][j : j + 1], (8, LANES))
                taps_out[a1, j] = jnp.where(odd, odd_row, even_row)

    def crossing(piece, source, target):
        return [
            pltpu.make_async_remote_copy(
                src_ref=source.at[flat(other, *at)],
                dst_ref=target.at[mine],
                send_sem=send_sem.at[piece],
                recv_sem=recv_sem.at[piece],
                device_id=named(other, *at),
                device_id_type=MESH,
            )
            for at in across
        ]

    def staying(piece, source, target):
        copies = []
        for dy, dc in BESIDE:
            to = (zh, lax.rem(y + dy, 4), lax.rem(c + dc, 2))
            copy = pltpu.make_async_remote_copy(
                src_ref=source.at[flat(*to)],
                dst_ref=target.at[mine],
                send_sem=send_sem.at[piece],
                recv_sem=recv_sem.at[piece + 3],
                device_id=named(*to),
                device_id_type=MESH,
            )
            copies.append(copy)
        return copies

    def whole(piece, target, count, near):
        return pltpu.make_async_remote_copy(
            src_ref=target.at[pl.ds(0, count)],
            dst_ref=target.at[pl.ds(0, count)],
            send_sem=send_sem.at[piece],
            recv_sem=recv_sem.at[piece + 3 * near],
            device_id=named(other, y, c),
            device_id_type=MESH,
        )

    def part(m, at):
        return pltpu.make_async_remote_copy(
            src_ref=sent.at[0, flat(other, *at), :, pl.ds(LANES * m, LANES)],
            dst_ref=early.at[mine, :, pl.ds(LANES * m, LANES)],
            send_sem=send_sem.at[0],
            recv_sem=recv_sem.at[0],
            device_id=named(other, *at),
            device_id_type=MESH,
        )

    zero = crossing(0, sent.at[0], early)
    one = crossing(1, sent.at[1], got)
    two = crossing(2, tails, heads)

    def start(copies):
        @pl.when(late)
        def _():
            for copy in copies:
                copy.start()

    loads[1].wait()
    delay(HEAD, HALF)
    loads[3].wait()
    compute(0, 0)
    start([part(0, at) for at in across[:4]])
    loads[2].wait()
    delay(HEAD + HALF, HALF + TAIL)
    compute(0, 1)
    start([part(1, at) for at in across[:4]])
    for load in loads[4:]:
        load.start()
    compute(1, 0)
    compute(1, 1)
    start(one[:4])

    ends = [coarse_frames(xs, ys, taps, ROWS + 2 * a1, 8) for a1 in range(2)]
    lower = lax.broadcasted_iota(jnp.int32, (8, 256), 0) < 4
    ends = jnp.where(lower, ends[0], pltpu.roll(ends[1], 4, 0))
    result = spectra(ms, jnp.concatenate([ends] * 16, axis=0))
    chosen = (
        lax.broadcasted_iota(jnp.int32, (16, LANES), 1) // 8
        == lax.broadcasted_iota(jnp.int32, (16, LANES), 0)
    )
    for d in range(PEERS):
        picked = jnp.where(chosen, result[16 * d : 16 * d + 16], 0.0)
        tails[d] = jnp.sum(picked, axis=0, keepdims=True)
    heads[mine] = tails[mine]
    start([*zero[4:], *two, *one[4:]])

    @pl.when(jnp.logical_not(late))
    def _():
        @pl.when(patient)
        def _():
            pl.semaphore_wait(barrier, 8)
            turned()

        for half in (slice(0, 4), slice(4, 8)):
            for at, copy in zip(across[half], zero[half], strict=True):
                pl.semaphore_wait(ready.at[flat(0, *at)], 1)
                copy.start()
            for copy in (*two[half], *one[half]):
                copy.start()
        @pl.when(jnp.logical_not(patient))
        def _():
            pl.semaphore_wait(barrier, 8)

        pl.semaphore_signal(again, inc=1, device_id=named(other, y, c), device_id_type=MESH)

    early[mine] = sent[0, mine]
    got[mine] = sent[1, mine]

    @pl.when(late)
    def _():
        pl.semaphore_wait(again, 1)

    near = [
        *staying(0, sent.at[0], early),
        *staying(2, tails, heads),
        *staying(1, sent.at[1], got),
    ]
    for copy in near:
        copy.start()

    @pl.when(jnp.logical_not(patient))
    def _():
        turned()

    sorted_taps()

    loads[5].wait()
    loads[6].wait()

    row = lax.rem(lax.broadcasted_iota(jnp.int32, (256, 256), 0), 8)
    column = lax.broadcasted_iota(jnp.int32, (256, 256), 1)
    lane = lax.rem(column, LANES)
    select = jnp.logical_and(lane < 4, row == column // LANES * 4 + lane)
    select = jnp.where(select, 1.0, 0.0).astype(jnp.bfloat16)

    def spread(half):
        some = slice(8 * half, 8 * half + 8)
        picked = [
            jnp.where(chosen, jnp.broadcast_to(heads[s], (16, LANES)), 0.0)
            for s in range(8 * half, 8 * half + 8)
        ]
        added = jnp.dot(
            jnp.concatenate(split(jnp.concatenate(picked, axis=0)), axis=1),
            select,
            preferred_element_type=jnp.float32,
        ).reshape(8, 16, 256)
        over_end[some] = added[:, :, :LANES]
        extra[some] = added[:, :, LANES:]

    def put(half, quarters, add):
        rows = slice(16 * half, 16 * half + 16)
        for d, both in enumerate(quarters):
            lanes = slice(LANES * d, LANES * d + LANES)
            for part, value in enumerate(both):
                value = value.reshape(4, 16, LANES)
                if add:
                    value = value + first[part, :, rows, lanes]
                first[part, :, rows, lanes] = value

    whole(0, early, 7, True).wait_recv()
    whole(1, got, 7, True).wait_recv()
    whole(2, heads, 7, True).wait_recv()

    @pl.when(late)
    def _():
        whole(2, heads, 8, False).wait_recv()
        spread(1)
        whole(0, early, 8, False).wait_recv()

    spread(0)
    put(0, classes(0, 0, 16, early, over_end, taps_out, fir, cm, tw), False)

    @pl.when(jnp.logical_not(late))
    def _():
        put(0, classes(1, 0, 16, got, extra, taps_out, fir, cm, tw), True)
        whole(2, heads, 8, False).wait_recv()
        spread(1)
        whole(0, early, 8, False).wait_recv()

    put(1, classes(0, 16, 16, early, over_end, taps_out, fir, cm, tw), False)
    whole(0, early, 15, True).wait_send()
    whole(2, heads, 15, True).wait_send()
    whole(1, got, 8, False).wait_recv()
    whole(1, got, 15, True).wait_send()


def fine_kernel(got, extra, taps, first, cm, tw, out, fir, stage, out_sem):
    late = lax.axis_index("zh") == 1

    def write(source, start, count, k):
        rows = pl.ds(start, count)
        return pltpu.make_async_copy(source.at[:, k, rows], out.at[:, k, rows], out_sem.at[k])

    def finish(start, count):
        rows = slice(start, start + count)
        quarters = classes(1, start, count, got, extra, taps, fir, cm, tw)
        for k in range(4):
            for d, both in enumerate(quarters):
                lanes = slice(LANES * d, LANES * d + LANES)
                for part, value in enumerate(both):
                    stage[part, k, rows, lanes] = (
                        first[part, k, rows, lanes] + value[count * k : count * (k + 1)]
                    )
            write(stage, start, count, k).start()

    @pl.when(jnp.logical_not(late))
    def _():
        for k in range(4):
            write(first, 0, 16, k).start()
        finish(16, 16)

    @pl.when(late)
    def _():
        finish(0, 32)

    for k in range(4):
        write(stage, 0, 32, k).wait()


def on_device(signal, coarse_taps, fine_taps):
    rows = signal.reshape(2, HALF, LANES).transpose(1, 0, 2).reshape(ROWS, LANES)
    hbm = pl.BlockSpec(memory_space=pltpu.HBM)
    vmem = pl.BlockSpec(memory_space=pltpu.VMEM)
    tables = [jnp.asarray(v) for v in (coarse_matrix(), fine_matrix(), twiddles())]
    operands = (rows, tables[0], coarse_taps, fine_taps, *tables[1:])
    f32 = jnp.float32
    handed = pl.pallas_call(
        gather_kernel,
        out_shape=[
            jax.ShapeDtypeStruct((PEERS, 16, 256), f32),
            jax.ShapeDtypeStruct((PEERS, 16, LANES), f32),
            jax.ShapeDtypeStruct((2, FINE_TAPS, 8, LANES), f32),
            jax.ShapeDtypeStruct((2, 4, 32, FINE), f32),
            jax.ShapeDtypeStruct((768, 256), jnp.bfloat16),
            jax.ShapeDtypeStruct((8, LANES), f32),
        ],
        in_specs=[hbm] * 6,
        out_specs=[vmem] * 6,
        scratch_shapes=[
            pltpu.VMEM((HEAD + ROWS + TAIL, LANES), f32),
            pltpu.VMEM((HEAD + ROWS + TAIL, LANES), f32),
            pltpu.VMEM((256, 512), jnp.bfloat16),
            pltpu.VMEM((TAPS, CHANNELS), f32),
            pltpu.VMEM((FINE_TAPS, FINE), f32),
            pltpu.VMEM((FINE, LANES), f32),
            pltpu.VMEM((PEERS, 16, 256), f32),
            pltpu.VMEM((PEERS, 1, LANES), f32),
            pltpu.VMEM((PEERS, 1, LANES), f32),
            pltpu.VMEM((2, PEERS, 16, 256), f32),
            pltpu.VMEM((PEERS, 16, LANES), f32),
            pltpu.VMEM((2, LANES, LANES), f32),
            pltpu.SemaphoreType.DMA((7,)),
            pltpu.SemaphoreType.DMA((3,)),
            pltpu.SemaphoreType.DMA((6,)),
            pltpu.SemaphoreType.REGULAR((8,)),
            pltpu.SemaphoreType.REGULAR,
        ],
        compiler_params=pltpu.CompilerParams(
            collective_id=0, has_side_effects=True, vmem_limit_bytes=16 << 20
        ),
        name="gather",
    )(*(pltpu.with_memory_space_constraint(v, pltpu.HBM) for v in operands))
    return pl.pallas_call(
        fine_kernel,
        out_shape=jax.ShapeDtypeStruct((2, 4, 32, FINE), f32),
        in_specs=[vmem] * 6,
        out_specs=hbm,
        scratch_shapes=[
            pltpu.VMEM((2, 256, LANES), f32),
            pltpu.VMEM((2, 4, 32, FINE), f32),
            pltpu.SemaphoreType.DMA((4,)),
        ],
        compiler_params=pltpu.CompilerParams(vmem_limit_bytes=16 << 20),
        name="fine",
    )(*handed)


def solution(mesh):
    finer = Mesh(mesh.devices.reshape(mesh.shape["streams"], *GROUP), ("streams", *TM))
    return jax.shard_map(
        on_device,
        mesh=finer,
        in_specs=(P(None, ("streams", *TM)), P(), P()),
        out_specs=P(None, TM, "streams", None),
        check_vma=False,
    )
```
